768 devices in a mesh: dom: 192 (over y, z, core), sub: 4 (over x).
Axes of the slice: x: 4, y: 8, z: 12, core: 2. Of those that a mesh axis runs over, the one named last changes fastest.
Arguments:
- fine_partial: float32 [4, 165, 24576], P('sub', None, 'dom'), may hold values from -6 to 6
- upward_ops: float32 [8, 165, 165], replicated, may hold values from -0.15625 to 0.15625
- interaction_ops: float32 [188, 165, 165], P('sub'), may hold values from -0.03125 to 0.03125
- downward_ops: float32 [8, 165, 165], replicated, may hold values from -0.5 to 0.5
- fine_list: int32 [188, 24576], P('sub', 'dom'), may hold values from -1 to 24575, as said below
- mid_list: int32 [188, 3072], P('sub', 'dom'), may hold values from -1 to 3071, as said below
- top_list: int32 [188, 384], P('sub', 'dom'), may hold values from -1 to 383, as said below
- upper_list: int32 [188, 48], P('sub'), may hold values from -1 to 47, as said below
- positions: float32 [3, 1572864], P(None, ('dom', 'sub')), may hold values from -0.5 to 0.5
- leaf_cell: int32 [1572864], P(('dom', 'sub')), may hold values from 0 to 24575, as said below
Outputs:
- local_fine: float32 [165, 24576], P(None, 'dom')
- potential: float32 [1572864], P(('dom', 'sub'))
The draws below stay inside these ranges and needn't reach their ends.
Inputs may be any that keep to these rules, and one draw needn't show every extreme that they name: `fine_list`: column t lists for each offset slot a cell of the finest level within 128 cells of t in Peano order, or -1 for an empty slot. `mid_list`: column t lists for each offset slot a cell of the middle level within 16 cells of t, or -1 for an empty slot. `top_list`: each entry is a cell of the top level, or -1 for an empty slot. `upper_list`: each entry is a cell of the upper level, or -1 for an empty slot. `leaf_cell`: A particle's leaf is one of the 128 finest cells owned by its own slab.
All inputs are finite; a program needn't handle non-finite values.
Results may differ from the reference program's by a relative error of at most 0.0003.
Values sent between devices are 32-bit elements; how exact they have to be, the bound alone decides.
No kernel may reach another device: no remote copies, remote signals or barrier semaphores. Data moves between devices by JAX's collectives and lax.ppermute only.
A program may use at most 128 MiB of HBM per device.

```python
import jax
import jax.numpy as jnp
from jax import lax

ORDER = 8
NC = 165
NOFF = 188
CF = 128
NF = 24576
NM = 3072
NT = 384
NU = 48
PARTICLES = 1572864
N_DOM = 192
N_SUB = 4


def window_list(key, cells_total, reach):
    targets = jnp.arange(cells_total, dtype=jnp.int32)[None, :]
    offsets = jax.random.randint(key, (NOFF, cells_total), -reach, reach + 1, dtype=jnp.int32)
    sources = targets + offsets
    inside = (sources >= 0) & (sources < cells_total)
    return jnp.where(inside, sources, -1).astype(jnp.int32)


def global_list(key, cells_total):
    key_one, key_two = jax.random.split(key)
    drawn_cells = jax.random.randint(key_one, (NOFF, cells_total), 0, cells_total, dtype=jnp.int32)
    vacant = jax.random.randint(key_two, (NOFF, cells_total), 0, 8, dtype=jnp.int32) == 0
    return jnp.where(vacant, -1, drawn_cells).astype(jnp.int32)


def draw_fine_list(key, part):
    return window_list(jax.random.fold_in(key, 11), NF, CF)


def draw_mid_list(key, part):
    return window_list(jax.random.fold_in(key, 12), NM, CF // 8)


def draw_top_list(key, part):
    return global_list(jax.random.fold_in(key, 13), NT)


def draw_upper_list(key, part):
    return global_list(jax.random.fold_in(key, 14), NU)


def draw_leaf_cell(key, part):
    slabs = NF // CF
    indices = jnp.arange(PARTICLES, dtype=jnp.int32)
    slab_index = indices // (PARTICLES // slabs)
    inner = jax.random.randint(jax.random.fold_in(key, 15), (PARTICLES,), 0, CF, dtype=jnp.int32)
    return (slab_index * CF + inner).astype(jnp.int32)


def level_of(stream_key, extent, shards, smallest, top_value):
    gain, own = 1.0, jax.random.fold_in(stream_key, 6)
    for position, blocks in shards:
        draws = jnp.exp(jax.random.uniform(jax.random.fold_in(own, position), (blocks,), jnp.float32, smallest / len(shards), top_value / len(shards)))
        gain = gain * jnp.repeat(draws, extent[position] // blocks).reshape([-1 if axis == position else 1 for axis in range(len(extent))])
    return gain


def noise(key, dims, scale, most, pieces=(), kind=jnp.bfloat16):
    result = scale * jax.random.normal(key, dims, jnp.float32)
    if pieces:
        result = result * level_of(key, dims, pieces, -0.22, 0.18)
    return jnp.clip(result, -most, most).astype(kind)


def setup_inputs(seed: int = 0) -> dict:
    splits = jax.random.split(jax.random.key(seed), 11)
    return {
        "fine_partial": noise(splits[0], (N_SUB, NC, NF), 1.0, 6.0, ((0, 4), (2, 192)), jnp.float32),
        "upward_ops": noise(splits[1], (8, NC, NC), (8 * NC) ** -0.5, 0.15625, (), jnp.float32),
        "interaction_ops": noise(splits[2], (NOFF, NC, NC), (NOFF * NC) ** -0.5, 0.03125, ((0, 4),), jnp.float32),
        "downward_ops": noise(splits[3], (8, NC, NC), NC ** -0.5, 0.5, (), jnp.float32),
        "fine_list": draw_fine_list(jax.random.fold_in(splits[10], 71), 0),
        "mid_list": draw_mid_list(jax.random.fold_in(splits[10], 71), 0),
        "top_list": draw_top_list(jax.random.fold_in(splits[10], 71), 0),
        "upper_list": draw_upper_list(jax.random.fold_in(splits[10], 71), 0),
        "positions": jnp.clip(jax.random.uniform(splits[8], (3, PARTICLES), jnp.float32, -0.5, 0.5) * level_of(splits[8], (3, PARTICLES), ((1, 768),), -0.4, 0.0), -0.5, 0.5),
        "leaf_cell": draw_leaf_cell(jax.random.fold_in(splits[10], 71), 0),
    }


precise = lax.Precision.HIGHEST


def exponents():
    entries = []
    for degree in range(ORDER + 1):
        for along_x in range(degree, -1, -1):
            for along_y in range(degree - along_x, -1, -1):
                entries.append((along_x, along_y, degree - along_x - along_y))
    return entries


def monomials(coords):
    powers = [jnp.ones_like(coords)]
    for degree in range(ORDER):
        powers.append(powers[-1] * coords)
    rows = []
    for triple in exponents():
        rows.append(powers[triple[0]][0] * powers[triple[1]][1] * powers[triple[2]][2])
    return jnp.stack(rows)


def upward(moments, upward_ops):
    parents = moments.shape[1] // 8
    grouped = moments.reshape(moments.shape[0], parents, 8)
    return jnp.einsum("oab,bpo->ap", upward_ops, grouped, precision=precise)


def downward(expansions, downward_ops):
    spread = jnp.einsum("oab,bp->apo", downward_ops, expansions, precision=precise)
    return spread.reshape(spread.shape[0], -1)


def interact(moments, sources, interaction_ops, block_size):
    targets = sources.shape[1]

    def one_block(block_index):
        chosen = lax.dynamic_slice_in_dim(sources, block_index * block_size, block_size, 1)
        present = chosen >= 0
        picked = jnp.take(moments, jnp.clip(chosen, 0, moments.shape[1] - 1), axis=1)
        picked = jnp.where(present[None], picked, jnp.float32(0.0))
        return jnp.einsum("jab,bjt->at", interaction_ops, picked, precision=precise)

    results = lax.map(one_block, jnp.arange(targets // block_size, dtype=jnp.int32))
    return jnp.transpose(results, (1, 0, 2)).reshape(moments.shape[0], targets)


def reference(fine_partial, upward_ops, interaction_ops, downward_ops, fine_list, mid_list, top_list, upper_list, positions, leaf_cell):
    fine_moments = jnp.sum(fine_partial, axis=0)
    mid_moments = upward(fine_moments, upward_ops)
    top_moments = upward(mid_moments, upward_ops)
    upper_moments = upward(top_moments, upward_ops)
    local_upper = interact(upper_moments, upper_list, interaction_ops, upper_moments.shape[1])
    local_top = interact(top_moments, top_list, interaction_ops, CF // 64) + downward(local_upper, downward_ops)
    local_mid = interact(mid_moments, mid_list, interaction_ops, CF // 8) + downward(local_top, downward_ops)
    local_fine = interact(fine_moments, fine_list, interaction_ops, CF) + downward(local_mid, downward_ops)
    slab_span = PARTICLES // N_DOM

    def slab_potential(slab_index):
        coords = lax.dynamic_slice_in_dim(positions, slab_index * slab_span, slab_span, 1)
        leaves = lax.dynamic_slice_in_dim(leaf_cell, slab_index * slab_span, slab_span, 0)
        columns = jnp.take(local_fine, leaves, axis=1)
        return jnp.sum(columns * monomials(coords), axis=0)

    potential = lax.map(slab_potential, jnp.arange(N_DOM, dtype=jnp.int32)).reshape(-1)
    return local_fine, potential
```

```python
import jax
import jax.numpy as jnp
from jax import lax
from jax.sharding import Mesh
from jax.sharding import PartitionSpec as P

ORDER = 8
DOM = ("dom_0", "dom_1", "dom_2")
DOM_SUB = ("dom_0", "dom_1", "dom_2", "sub")


precise = lax.Precision.HIGHEST


def sent_to_all(value, axis):
    copies = jnp.broadcast_to(value, (lax.axis_size(axis), *value.shape))
    return lax.all_to_all(copies, axis, split_axis=0, concat_axis=0, tiled=True)


def taken_together(value, axis):
    everything = sent_to_all(value, axis)
    return jnp.sum(everything, axis=0)


def extended(block, sides, width):
    for axis, dim in sides:
        count = lax.axis_size(axis)
        forward = [(i, i + 1) for i in range(count - 1)]
        backward = [(target, source) for source, target in forward]
        low = lax.ppermute(
            lax.slice_in_dim(block, block.shape[dim] - width, None, axis=dim), axis, forward
        )
        high = lax.ppermute(lax.slice_in_dim(block, 0, width, axis=dim), axis, backward)
        block = jnp.concatenate([low, block, high], axis=dim)
    return block


def exponents():
    entries = []
    for degree in range(ORDER + 1):
        for along_x in range(degree, -1, -1):
            for along_y in range(degree - along_x, -1, -1):
                entries.append((along_x, along_y, degree - along_x - along_y))
    return entries


def monomial_rows(coords):
    powers = [jnp.ones_like(coords)]
    for degree in range(ORDER):
        powers.append(powers[-1] * coords)
    rows = []
    for triple in exponents():
        rows.append(powers[triple[0]][0] * powers[triple[1]][1] * powers[triple[2]][2])
    return jnp.stack(rows, axis=1)


def upward(moments, upward_ops):
    parents = moments.shape[1] // 8
    grouped = moments.reshape(moments.shape[0], parents, 8)
    return jnp.einsum("oab,bpo->ap", upward_ops, grouped, precision=precise)


def downward(expansions, downward_ops):
    spread = jnp.einsum("oab,bp->apo", downward_ops, expansions, precision=precise)
    return spread.reshape(spread.shape[0], -1)


def interact_local(moments, sources, anchor, flat_ops):
    coeffs, columns = moments.shape
    cell_rows = jnp.concatenate(
        [jnp.transpose(moments), jnp.zeros((1, coeffs), jnp.float32)], axis=0
    )
    shifted = jnp.where(sources >= 0, jnp.clip(sources - anchor, 0, columns - 1), columns)
    picked = jnp.take(cell_rows, jnp.transpose(shifted), axis=0)
    stacked = picked.reshape(picked.shape[0], picked.shape[1] * picked.shape[2])
    result = jnp.dot(stacked, flat_ops, precision=precise, preferred_element_type=jnp.float32)
    return jnp.transpose(result)


def settle(portion, each_level):
    if each_level:
        return taken_together(portion, "sub")
    return portion


def shards(
    fine_partial,
    upward_ops,
    interaction_ops,
    downward_ops,
    fine_list,
    mid_list,
    top_list,
    upper_list,
    positions,
    leaf_cell,
):
    slab_cells = fine_partial.shape[2]
    mid_cells = slab_cells // 8
    top_cells = slab_cells // 64
    domain = lax.axis_index(DOM)
    coeffs = interaction_ops.shape[1]
    flat_ops = jnp.transpose(interaction_ops, (0, 2, 1)).reshape(-1, coeffs)
    fine_moments = taken_together(fine_partial[0], "sub")
    wide_fine = extended(fine_moments, ((DOM, 1),), slab_cells)
    wide_mid = upward(wide_fine, upward_ops)
    mid_moments = wide_mid[:, mid_cells : 2 * mid_cells]
    own_top = upward(mid_moments, upward_ops)
    pieces = sent_to_all(jnp.transpose(own_top), ("dom_1", "dom_2"))
    pieces = sent_to_all(pieces, "dom_0")
    top_moments = jnp.transpose(pieces.reshape(-1, coeffs))
    upper_moments = upward(top_moments, upward_ops)
    upper_span = max(1, top_cells // 8)
    upper_first = domain * top_cells // 8
    upper_sources = lax.dynamic_slice_in_dim(upper_list, upper_first, upper_span, 1)
    local_upper = settle(interact_local(upper_moments, upper_sources, 0, flat_ops), False)
    down_top = downward(local_upper, downward_ops)
    top_offset = domain * top_cells % 8
    local_top = settle(interact_local(top_moments, top_list, 0, flat_ops), False)
    local_top = local_top + lax.dynamic_slice_in_dim(down_top, top_offset, top_cells, 1)
    local_mid = settle(
        interact_local(wide_mid, mid_list, domain * mid_cells - mid_cells, flat_ops), False
    )
    local_mid = local_mid + downward(local_top, downward_ops)
    local_fine = settle(
        interact_local(wide_fine, fine_list, domain * slab_cells - slab_cells, flat_ops), False
    )
    local_fine = local_fine + downward(local_mid, downward_ops)
    local_fine = settle(local_fine, True)
    fine_rows = jnp.transpose(local_fine)
    leaves = leaf_cell - domain * slab_cells
    particles = positions.shape[1]
    block_size = min(particles, 4096)

    def evaluate(block_index):
        picked = jnp.take(fine_rows, leaves, axis=0)
        return jnp.sum(picked * monomial_rows(positions), axis=1)

    potential = lax.map(evaluate, jnp.arange(particles // block_size, dtype=jnp.int32)).reshape(-1)
    return (local_fine, potential)


def solution(mesh):
    torus = Mesh(
        mesh.devices.reshape(8, 12, 2, mesh.shape["sub"]), ("dom_0", "dom_1", "dom_2", "sub")
    )
    return jax.shard_map(
        shards,
        mesh=torus,
        in_specs=(
            P("sub", None, DOM),
            P(),
            P("sub", None, None),
            P(),
            P("sub", DOM),
            P("sub", DOM),
            P("sub", DOM),
            P("sub", None),
            P(None, DOM_SUB),
            P(DOM_SUB),
        ),
        out_specs=(P(None, DOM), P(DOM_SUB)),
        check_vma=False,
    )
```

```python
import jax
import jax.numpy as jnp
from jax import lax
from jax.experimental import pallas as pl
from jax.experimental.pallas import tpu as pltpu
from jax.sharding import Mesh
from jax.sharding import PartitionSpec as P

ORDER = 8
F32, BF16, I32 = jnp.float32, jnp.bfloat16, jnp.int32
VMEM = pltpu.VMEM


def split(value):
    high = value.astype(BF16)
    return high, (value - high.astype(F32)).astype(BF16)


def halves(pair):
    return pair[:, :128] + pair[:, 128:]


def mm(a, b):
    return jnp.dot(a, b, preferred_element_type=F32)


def mm_nt(a, b):
    return lax.dot_general(a, b, (((1,), (1,)), ((), ())), preferred_element_type=F32)


def gathered(high, low, chosen):
    return jnp.concatenate([mm(high, chosen).astype(BF16), mm(low, chosen).astype(BF16)], axis=1)


def child_picker(rows, octant):
    r = lax.broadcasted_iota(I32, (rows, 128), 0)
    c = lax.broadcasted_iota(I32, (rows, 128), 1)
    return (r == 8 * c + octant).astype(F32).astype(BF16)


def child_spreader(octant):
    r = lax.broadcasted_iota(I32, (128, 128), 0)
    c = lax.broadcasted_iota(I32, (128, 128), 1)
    return (c == 8 * r + octant).astype(F32).astype(BF16)


def raised(moments, uph, upl, rows):
    high, low = split(moments)
    total = None
    for o in range(8):
        picked = gathered(high, low, child_picker(rows, o))
        term = mm(uph[o], picked) + mm(upl[o], picked)
        total = term if total is None else total + term
    return halves(total)


def lowered(expansion, dnh, dnl):
    high, low = split(expansion)
    total = None
    for o in range(8):
        spread = gathered(high, low, child_spreader(o))
        term = mm(dnh[o], spread) + mm(dnl[o], spread)
        total = term if total is None else total + term
    return halves(total)


def split_ops_kernel(up_ref, down_ref, uph, upl, dnh, dnl):
    for o in range(8):
        uph[o], upl[o] = split(up_ref[:, o, :])
        dnh[o], dnl[o] = split(down_ref[:, o, :])


def split_ops(upward_ops, downward_ops):
    n = upward_ops.shape[1]
    shape = jax.ShapeDtypeStruct((8, n, n), BF16)
    return pl.pallas_call(
        split_ops_kernel,
        out_shape=(shape,) * 4,
        in_specs=[pl.BlockSpec(memory_space=VMEM)] * 2,
        out_specs=(pl.BlockSpec(memory_space=VMEM),) * 4,
        compiler_params=pltpu.CompilerParams(vmem_limit_bytes=16 << 20),
        name="split_ops",
    )(jnp.transpose(upward_ops, (1, 0, 2)), jnp.transpose(downward_ops, (1, 0, 2)))


def own_kernel(parts, uph, upl, fine_ref, top_ref):
    fine = parts[0] + parts[1] + parts[2] + parts[3]
    fine_ref[...] = fine
    mid = raised(fine, uph, upl, 128)
    top = raised(mid, uph, upl, 128)
    rows = jnp.transpose(top)[:2]
    for i in range(top_ref.shape[0]):
        top_ref[i] = rows


def own_moments(parts, uph, upl, copies):
    n = parts.shape[1]
    return pl.pallas_call(
        own_kernel,
        out_shape=(jax.ShapeDtypeStruct((n, 128), F32), jax.ShapeDtypeStruct((copies, 2, n), F32)),
        in_specs=[pl.BlockSpec(memory_space=VMEM)] * 3,
        out_specs=(pl.BlockSpec(memory_space=VMEM),) * 2,
        compiler_params=pltpu.CompilerParams(vmem_limit_bytes=16 << 20),
        name="own_moments",
    )(parts, uph, upl)


GROUP = 8


def near_kernel(place, left, own, right, uph, upl, fl, ml, ops, fine_out, mid_out, wide, mids, xs, acc_a, acc_b):
    slots, n = ops.shape[0], ops.shape[1]
    for i, ref in enumerate((left, own, right)):
        wide[0, :, pl.ds(128 * i, 128)], wide[1, :, pl.ds(128 * i, 128)] = split(ref[...])
    total = None
    for o in range(8):
        picked = gathered(wide[0], wide[1], child_picker(384, o))
        term = mm(uph[o], picked) + mm(upl[o], picked)
        total = term if total is None else total + term
    mids[:, pl.ds(0, 128)], mids[:, pl.ds(128, 128)] = split(halves(total))
    anchor = place[0] * 128 - 128
    mid_anchor = place[0] * 16 - 16
    lane = lax.broadcasted_iota(I32, (1, 128), 1)
    part = (lane // 16) % 2 * 128
    acc_a[...] = jnp.zeros_like(acc_a)
    acc_b[...] = jnp.zeros_like(acc_b)

    def load(g, count):
        for q in range(0, count, 4):
            row = ml[pl.ds((g + q) // 4, 1), :]
            row = jnp.where(row >= 0, row - mid_anchor + part, -1)
            source = lax.broadcasted_iota(I32, (256, 128), 0)
            tile = mm(mids[...], (source == row).astype(F32).astype(BF16)).astype(BF16)
            for jj in range(q, min(q + 4, count)):
                xs[jj, :, pl.ds(128, 128)] = jnp.where(lane // 32 == jj - q, tile, jnp.zeros_like(tile))
        for q in range(0, count, 2):
            rows = []
            for jj in range(q, min(q + 2, count)):
                row = fl[pl.ds(g + jj, 1), :]
                rows.append(jnp.where(row >= 0, row - anchor, -1))
            row = jnp.concatenate(rows, axis=1)
            source = lax.broadcasted_iota(I32, (384, row.shape[1]), 0)
            chosen = (source == row).astype(F32).astype(BF16)
            for h in range(2):
                got = mm(wide[h], chosen).astype(BF16)
                for i in range(len(rows)):
                    xs[q + i, :, pl.ds(256 * h, 128)] = got[:, 128 * i : 128 * (i + 1)]

    def use(g, count):
        a = b = None
        for jj in range(count):
            oh, ol = split(ops[g + jj])
            x = xs[jj]
            ta = mm(oh, x[:, :256]) + mm(ol, x[:, :256])
            tb = mm(oh, x[:, 256:])
            a = ta if a is None else a + ta
            b = tb if b is None else b + tb
        acc_a[...] += a
        acc_b[...] += b

    for g in range(0, slots, GROUP):
        count = min(GROUP, slots - g)
        load(g, count)
        use(g, count)
    fine_out[...] = acc_a[:, pl.ds(0, 128)] + acc_b[...]
    folded = acc_a[:, pl.ds(128, 128)]
    for shift in (64, 32, 16):
        folded = folded + pltpu.roll(folded, shift, 1)
    mid_out[...] = folded


def near_terms(place, left, own, right, uph, upl, fine_list, mid_rows, ops):
    n = ops.shape[1]
    vm = pl.BlockSpec(memory_space=VMEM)
    return pl.pallas_call(
        near_kernel,
        out_shape=(jax.ShapeDtypeStruct((n, 128), F32),) * 2,
        in_specs=[pl.BlockSpec(memory_space=pltpu.SMEM)] + [vm] * 8,
        out_specs=(vm,) * 2,
        scratch_shapes=[
            pltpu.VMEM((2, n, 384), BF16),
            pltpu.VMEM((n, 256), BF16),
            pltpu.VMEM((GROUP, n, 384), BF16),
            pltpu.VMEM((n, 256), F32),
            pltpu.VMEM((n, 128), F32),
        ],
        compiler_params=pltpu.CompilerParams(vmem_limit_bytes=12 << 20),
        name="near_terms",
    )(place, left, own, right, uph, upl, fine_list, mid_rows, ops)


def far_kernel(
    place, tl, ul, table, uph, upl, dnh, dnl, fine_term, mid_term, ops, out,
    rows, upper, chosen, top_col, upper_col,
):
    slots, n = ops.shape[0], ops.shape[1]
    parents = rows.shape[1] - 8
    rows[:, pl.ds(parents, 8), :] = jnp.zeros((8, 8, n), F32)
    upper[...] = jnp.zeros_like(upper)
    for a in range(table.shape[0]):
        for b in range(table.shape[1]):
            for i in range(2):
                cell = (a * table.shape[1] + b) * 2 + i
                rows[cell % 8, pl.ds(cell // 8, 1), :] = table[a, b, pl.ds(i, 1), :]
    total = None
    for o in range(8):
        high, low = split(rows[o, pl.ds(0, parents), :])
        term = mm_nt(high, uph[o]) + mm_nt(high, upl[o]) + mm_nt(low, uph[o])
        total = term if total is None else total + term
    upper[pl.ds(0, parents), :] = total
    parent = place[0] // 4
    for j in range(slots):
        for t in range(2):
            index = tl[t, j]
            index = jnp.where(index >= 0, index, parents * 8)
            chosen[3 * j + t] = jnp.broadcast_to(rows[index & 7, pl.ds(index >> 3, 1), :], (8, n))
        index = ul[j, parent]
        index = jnp.where(index >= 0, index, parents)
        chosen[3 * j + 2] = jnp.broadcast_to(upper[pl.ds(index, 1), :], (8, n))
    lane = lax.broadcasted_iota(I32, (8, 128), 1)

    def block(start, size):
        sums = [jnp.zeros((size, n), F32)] * 3
        for j in range(slots):
            piece = ops[j, pl.ds(start, size), :]
            for t in range(3):
                sums[t] = sums[t] + piece * chosen[3 * j + t, :size]
        s0, s1, s2 = [jnp.sum(s, axis=1, keepdims=True) for s in sums]
        here = lane[:size]
        top_col[pl.ds(start, size), :] = jnp.where(here == 0, s0, jnp.where(here == 1, s1, 0.0))
        upper_col[pl.ds(start, size), :] = jnp.where(here < 2, s2, 0.0)

    def step(i, carry):
        block(pl.multiple_of(i * 8, 8), 8)
        return carry

    lax.fori_loop(0, n // 8, step, 0)
    if n % 8:
        block(n // 8 * 8, n % 8)
    both = jnp.concatenate(split(upper_col[...]), axis=1)
    octant = lax.rem(place[0] * 2, 8)
    lane = lax.broadcasted_iota(I32, (n, 128), 1)
    from_upper = [halves(mm(dnh[octant + i], both) + mm(dnl[octant + i], both)) for i in range(2)]
    local_top = top_col[...] + jnp.where(lane == 0, from_upper[0], jnp.where(lane == 1, from_upper[1], 0.0))
    local_mid = lowered(local_top, dnh, dnl) + mid_term[...]
    local_mid = jnp.where(lane < 16, local_mid, 0.0)
    local_fine = lowered(local_mid, dnh, dnl) + fine_term[...]
    for i in range(out.shape[0]):
        out[i] = local_fine


def far_terms(place, top_list, upper_list, table, uph, upl, dnh, dnl, fine_term, mid_term, ops, copies):
    slots, n = ops.shape[0], ops.shape[1]
    cells = table.shape[0] * table.shape[1] * 2
    vm, sm = pl.BlockSpec(memory_space=VMEM), pl.BlockSpec(memory_space=pltpu.SMEM)
    return pl.pallas_call(
        far_kernel,
        out_shape=jax.ShapeDtypeStruct((copies, n, 128), F32),
        in_specs=[sm] * 3 + [vm] * 8,
        out_specs=vm,
        scratch_shapes=[
            pltpu.VMEM((8, cells // 8 + 8, n), F32),
            pltpu.VMEM((cells // 8 + 8, n), F32),
            pltpu.VMEM((3 * slots, 8, n), F32),
            pltpu.VMEM((n, 128), F32),
            pltpu.VMEM((n, 128), F32),
        ],
        compiler_params=pltpu.CompilerParams(vmem_limit_bytes=12 << 20),
        name="far_terms",
    )(place, jnp.transpose(top_list), upper_list, table, uph, upl, dnh, dnl, fine_term, mid_term, ops)


def exponents():
    entries = []
    for degree in range(ORDER + 1):
        for along_x in range(degree, -1, -1):
            for along_y in range(degree - along_x, -1, -1):
                entries.append((along_x, along_y, degree - along_x - along_y))
    return entries


def monomial_kernel(powers, coords, high_ref, low_ref):
    n = powers.shape[0]
    terms = []
    value = None
    for axis in range(3):
        e = powers[:, pl.ds(axis, 1)]
        base = coords[pl.ds(axis, 1), :]
        for bit in range(4):
            factor = jnp.where((e >> bit) & 1 == 1, base, 1.0)
            value = factor if value is None else value * factor
            base = base * base
    high_ref[...], low_ref[...] = split(value)


def monomials(coords):
    table = jnp.asarray(exponents(), I32)
    n, particles = table.shape[0], coords.shape[1]
    width = 512
    return pl.pallas_call(
        monomial_kernel,
        grid=(particles // width,),
        out_shape=(jax.ShapeDtypeStruct((n, particles), BF16),) * 2,
        in_specs=[pl.BlockSpec((n, 3), lambda i: (0, 0)), pl.BlockSpec((3, width), lambda i: (0, i))],
        out_specs=(pl.BlockSpec((n, width), lambda i: (0, i)),) * 2,
        name="monomials",
    )(table, coords)


def potential_kernel(parts, leaves, high_ref, low_ref, fine_ref, out):
    fine = parts[0] + parts[1] + parts[2] + parts[3]
    fine_ref[...] = fine
    fh, fl = split(jnp.transpose(fine))
    width = 512
    cell = lax.broadcasted_iota(I32, (128, width), 0)
    for k in range(out.shape[1] // width):
        at = pl.ds(k * width, width)
        mh, ml = high_ref[:, at], low_ref[:, at]
        values = mm(fh, mh) + mm(fl, mh) + mm(fh, ml)
        out[:, at] = jnp.sum(jnp.where(cell == leaves[:, at], values, 0.0), axis=0, keepdims=True)


def potentials(parts, leaves, high, low):
    n = parts.shape[1]
    particles = leaves.shape[1]
    vm = pl.BlockSpec(memory_space=VMEM)
    return pl.pallas_call(
        potential_kernel,
        out_shape=(jax.ShapeDtypeStruct((n, 128), F32), jax.ShapeDtypeStruct((1, particles), F32)),
        in_specs=[vm] * 4,
        out_specs=(vm,) * 2,
        compiler_params=pltpu.CompilerParams(vmem_limit_bytes=16 << 20),
        name="potentials",
    )(parts, leaves, high, low)


DOM = ("dom_0", "dom_1", "dom_2")
DOM_SUB = ("dom_0", "dom_1", "dom_2", "sub")


def exchanged(copies, axes):
    return lax.all_to_all(copies, axes, split_axis=0, concat_axis=0, tiled=True)


def copied(value, count):
    return jnp.broadcast_to(value, (count, *value.shape))


def shards(
    fine_partial,
    upward_ops,
    interaction_ops,
    downward_ops,
    fine_list,
    mid_list,
    top_list,
    upper_list,
    positions,
    leaf_cell,
):
    slab_cells = fine_partial.shape[2]
    slots = interaction_ops.shape[0]
    subs, slabs = lax.axis_size("sub"), lax.axis_size(DOM)
    domain = lax.axis_index(DOM)
    place = domain.astype(I32).reshape(1)
    uph, upl, dnh, dnl = split_ops(upward_ops, downward_ops)
    parts = exchanged(copied(fine_partial[0], subs), "sub")
    own, tops = own_moments(parts, uph, upl, lax.axis_size(DOM[1:]))
    forward = [(i, i + 1) for i in range(slabs - 1)]
    backward = [(target, source) for source, target in forward]
    left = lax.ppermute(own, DOM, forward)
    right = lax.ppermute(own, DOM, backward)
    line = exchanged(tops, DOM[1:])
    table = exchanged(copied(line, lax.axis_size(DOM[0])), DOM[0])
    rows = -(-slots // 4)
    mid_rows = jnp.pad(mid_list, ((0, rows * 4 - slots), (0, 0)), constant_values=-1)
    mid_rows = jnp.concatenate([mid_rows, mid_rows], axis=1).reshape(rows, 128)
    fine_term, mid_term = near_terms(place, left, own, right, uph, upl, fine_list, mid_rows, interaction_ops)
    partial = far_terms(
        place, top_list, upper_list, table, uph, upl, dnh, dnl, fine_term, mid_term, interaction_ops, subs
    )
    high, low = monomials(positions)
    leaves = (leaf_cell - domain * slab_cells).reshape(1, -1)
    local_fine, potential = potentials(exchanged(partial, "sub"), leaves, high, low)
    return local_fine, potential.reshape(-1)


def solution(mesh):
    torus = Mesh(
        mesh.devices.reshape(8, 12, 2, mesh.shape["sub"]), ("dom_0", "dom_1", "dom_2", "sub")
    )
    return jax.shard_map(
        shards,
        mesh=torus,
        in_specs=(
            P("sub", None, DOM),
            P(),
            P("sub", None, None),
            P(),
            P("sub", DOM),
            P("sub", DOM),
            P("sub", DOM),
            P("sub", None),
            P(None, DOM_SUB),
            P(DOM_SUB),
        ),
        out_specs=(P(None, DOM), P(DOM_SUB)),
        check_vma=False,
    )
```

```python
import jax
import jax.numpy as jnp
from jax import lax
from jax.experimental import pallas as pl
from jax.experimental.pallas import tpu as pltpu
from jax.sharding import Mesh
from jax.sharding import PartitionSpec as P


ORDER = 8
F32, BF16, I32 = jnp.float32, jnp.bfloat16, jnp.int32
VMEM = pltpu.VMEM


def split(value):
    high = value.astype(BF16)
    return high, (value - high.astype(F32)).astype(BF16)


def in_hbm(value):
    return pltpu.with_memory_space_constraint(value, pltpu.HBM)


def halves(pair):
    return pair[:, :128] + pair[:, 128:]


def mm(a, b):
    return jnp.dot(a, b, preferred_element_type=F32)


def mm_nt(a, b):
    return lax.dot_general(a, b, (((1,), (1,)), ((), ())), preferred_element_type=F32)


def gathered(high, low, chosen):
    return jnp.concatenate([mm(high, chosen).astype(BF16), mm(low, chosen).astype(BF16)], axis=1)


def ones_where(shape, test):
    rows = lax.broadcasted_iota(I32, shape, 0)
    lanes = lax.broadcasted_iota(I32, shape, 1)
    return test(rows, lanes).astype(F32).astype(BF16)


def octant_sum(high, low, pair):
    lane = lax.broadcasted_iota(I32, (1, 256), 1) % 8
    total = None
    for o in range(8):
        term = mm(high[o], pair) + mm(low[o], pair)
        total = jnp.where(lane == o, term, 0.0 if total is None else total)
    return halves(total)


def raised(moments, uph, upl):
    summed = octant_sum(uph, upl, jnp.concatenate(split(moments), axis=1))
    parent = ones_where((128, 128), lambda r, c: r // 8 == c)
    high, low = split(summed)
    return mm(high, parent) + mm(low, parent)


def lowered(expansion, dnh, dnl):
    child = ones_where((128, 128), lambda r, c: c // 8 == r)
    return octant_sum(dnh, dnl, gathered(*split(expansion), child))


def split_kernel(ops_hbm, high, low, parts, sems):
    copies = [pltpu.make_async_copy(ops_hbm.at[:, o, :], parts.at[o], sems.at[o]) for o in range(8)]
    for copy in copies:
        copy.start()
    for o in range(8):
        copies[o].wait()
        high[o], low[o] = split(parts[o])


def split_ops(ops, kept=VMEM):
    n = ops.shape[1]
    return pl.pallas_call(
        split_kernel,
        out_shape=(kept((8, n, n), BF16),) * 2,
        in_specs=[pl.BlockSpec(memory_space=pltpu.HBM)],
        out_specs=(pl.BlockSpec(memory_space=VMEM),) * 2,
        scratch_shapes=[pltpu.VMEM((8, n, n), F32), pltpu.SemaphoreType.DMA((8,))],
        compiler_params=pltpu.CompilerParams(vmem_limit_bytes=8 << 20),
    )(in_hbm(jnp.transpose(ops, (1, 0, 2))))


MID_AT = 168
SHIFT = 64


def packed(first, second):
    n = first.shape[1]
    blank = jnp.zeros((1, SHIFT - (n - 128)), F32)
    rests = jnp.concatenate([first[:, 128:], blank, second[:, 128:], blank], axis=1)
    return jnp.concatenate([first[:, :128], rests, second[:, :128]], axis=1)


def own_kernel(parts, uph, upl, own_ref, top_ref):
    n = parts.shape[1]
    fine = (parts[0] + parts[1] + parts[2] + parts[3])[:, 0, :]
    own_ref[pl.ds(0, n), :] = fine
    mid = raised(fine, uph, upl)
    rows = jnp.transpose(mid)[:16]
    own_ref[pl.ds(MID_AT, 16), :] = rows[:, :128]
    own_ref[pl.ds(MID_AT + 16, 16), pl.ds(0, n - 128)] = rows[:, 128:]
    rows = jnp.transpose(raised(mid, uph, upl))
    row = packed(rows[:1], rows[1:2])
    for i in range(top_ref.shape[0]):
        top_ref[i] = row


def own_moments(parts, uph, upl, copies):
    return pl.pallas_call(
        own_kernel,
        out_shape=(VMEM((MID_AT + 32, 128), F32), VMEM((copies, 1, 384), F32)),
        in_specs=[pl.BlockSpec(memory_space=VMEM)] * 3,
        out_specs=(pl.BlockSpec(memory_space=VMEM),) * 2,
        compiler_params=pltpu.CompilerParams(vmem_limit_bytes=4 << 20),
        name="own_moments",
    )(parts, uph, upl)


def line_kernel(line, out):
    rows = line[:, 0, :]
    for i in range(out.shape[0]):
        out[i] = rows


def line_copies(line, copies):
    return pl.pallas_call(
        line_kernel,
        out_shape=jax.ShapeDtypeStruct((copies, line.shape[0], line.shape[2]), F32),
        in_specs=[pl.BlockSpec(memory_space=VMEM)],
        out_specs=pl.BlockSpec(memory_space=VMEM),
        compiler_params=pltpu.CompilerParams(vmem_limit_bytes=2 << 20),
        name="line_copies",
    )(line)


GROUP = 4


def near_kernel(place, left, own, right, fl, ml, ops_hbm, fine_out, mid_out, ops, full, rows, mids, mid_rows, xa, xb, acc_a, acc_b, sems):
    slots, n = ops.shape[0], ops.shape[1]
    groups = -(-slots // GROUP)
    size = [min(GROUP, slots - k * GROUP) for k in range(groups)]
    copies = []
    for k in range(0, groups, 2):
        at = pl.ds(k * GROUP, sum(size[k : k + 2]))
        copies.append(pltpu.make_async_copy(ops_hbm.at[at], ops.at[at], sems.at[k // 2]))
        copies[-1].start()
    rows[...] = jnp.zeros_like(rows)
    for i, ref in enumerate((left, own, right)):
        full[i] = ref[pl.ds(0, n), :]
        rows[pl.ds(16 * i, 16), pl.ds(0, 128)] = ref[pl.ds(MID_AT, 16), :]
        rows[pl.ds(16 * i, 16), pl.ds(128, n - 128)] = ref[pl.ds(MID_AT + 16, 16), pl.ds(0, n - 128)]
    mid = jnp.transpose(rows[...])[:n]
    mids[:, pl.ds(0, 128)], mids[:, pl.ds(128, 128)] = split(mid)
    anchor = place[0] * 128 - 128
    mid_anchor = place[0] * 16 - 16
    lane = lax.broadcasted_iota(I32, (1, 128), 1)
    part = (lane // 16) % 2 * 128
    listed = ml[...]
    listed = jnp.where(listed >= 0, listed - mid_anchor, -1).astype(F32).astype(BF16)
    spread = ones_where((16, 128), lambda r, c: c % 16 == r)
    mid_rows[...] = lax.dot_general(listed, spread, (((0,), (0,)), ((), ())), preferred_element_type=F32).astype(I32)
    acc_a[...] = jnp.zeros_like(acc_a)
    acc_b[...] = jnp.zeros_like(acc_b)

    def load(k, count, xs):
        row = jnp.full((1, 128), -1, I32)
        for jj in range(count):
            row = jnp.where(lane // 32 == jj, mid_rows[pl.ds(k * GROUP + jj, 1), :], row)
        row = jnp.where(row >= 0, row + part, -1)
        source = lax.broadcasted_iota(I32, (256, 128), 0)
        tile = mm(mids[...], (source == row).astype(F32).astype(BF16)).astype(BF16)
        for jj in range(count):
            xs[jj, :, pl.ds(128, 128)] = jnp.where(lane // 32 == jj, tile, jnp.zeros_like(tile))
            row = fl[pl.ds(k * GROUP + jj, 1), :]
            row = jnp.where(row >= 0, row - anchor, 512)
            index = jnp.broadcast_to(row & 127, (n, 128))
            got = jnp.zeros((n, 128), F32)
            for i in range(3):
                moved = jnp.take_along_axis(full[i], index, axis=1, mode="promise_in_bounds")
                got = jnp.where(row >> 7 == i, moved, got)
            xs[jj, :, pl.ds(0, 128)], xs[jj, :, pl.ds(256, 128)] = split(got)

    def use(k, count, xs):
        a = b = None
        for jj in range(count):
            oh, ol = split(ops[k * GROUP + jj])
            x = xs[jj]
            ta = mm(oh, x[:, :256]) + mm(ol, x[:, :256])
            tb = mm(oh, x[:, 256:])
            a = ta if a is None else a + ta
            b = tb if b is None else b + tb
        acc_a[...] += a
        acc_b[...] += b

    load(0, GROUP, xa)

    def ready(i):
        at = pl.ds(0, 2 * GROUP)
        if isinstance(i, int):
            copies[i].wait()
        else:
            pltpu.make_async_copy(ops_hbm.at[at], ops.at[at], sems.at[i]).wait()

    def step(i, carry):
        ready(i)
        load(2 * i + 1, GROUP, xb)
        use(2 * i, GROUP, xa)
        load(2 * i + 2, GROUP, xa)
        use(2 * i + 1, GROUP, xb)
        return carry

    steady = groups // 2 - 1
    lax.fori_loop(0, steady, step, 0)
    bufs = (xa, xb)
    for k in range(2 * steady, groups):
        if k % 2 == 0:
            ready(k // 2)
        if k + 1 < groups:
            load(k + 1, size[k + 1], bufs[(k + 1) % 2])
        use(k, size[k], bufs[k % 2])
    fine_out[...] = acc_a[:, pl.ds(0, 128)] + acc_b[...]
    folded = acc_a[:, pl.ds(128, 128)]
    for shift in (64, 32, 16):
        folded = folded + pltpu.roll(folded, shift, 1)
    mid_out[...] = folded


def near_terms(place, left, own, right, fine_list, mid_list, ops):
    slots, n = ops.shape[0], ops.shape[1]
    vm = pl.BlockSpec(memory_space=VMEM)
    return pl.pallas_call(
        near_kernel,
        out_shape=(VMEM((n, 128), F32),) * 2,
        in_specs=[pl.BlockSpec(memory_space=pltpu.SMEM)] + [vm] * 5 + [pl.BlockSpec(memory_space=pltpu.HBM)],
        out_specs=(vm,) * 2,
        scratch_shapes=[
            pltpu.VMEM((slots, n, n), F32),
            pltpu.VMEM((3, n, 128), F32),
            pltpu.VMEM((128, 256), F32),
            pltpu.VMEM((n, 256), BF16),
            pltpu.VMEM((slots, 128), I32),
            pltpu.VMEM((GROUP, n, 384), BF16),
            pltpu.VMEM((GROUP, n, 384), BF16),
            pltpu.VMEM((n, 256), F32),
            pltpu.VMEM((n, 128), F32),
            pltpu.SemaphoreType.DMA((-(-slots // (2 * GROUP)),)),
        ],
        compiler_params=pltpu.CompilerParams(vmem_limit_bytes=20 << 20),
        name="near_terms",
    )(place, left, own, right, fine_list, jnp.transpose(mid_list), in_hbm(ops))


TALL = 24
FIRST = (3, 2, 2)


def far_kernel(
    place, tl, ul, table, uph, upl, fine_term, mid_term, dnh_hbm, dnl_hbm, ops_hbm, out,
    ops, dnh, dnl, tiles, rows, upper, chosen, top_col, upper_col, sems, down_sems,
):
    slots, n = ops.shape[0], ops.shape[1]
    loads = []
    for k, at in enumerate(range(0, n, TALL)):
        where = (slice(None), pl.ds(at, min(TALL, n - at)))
        loads.append(pltpu.make_async_copy(ops_hbm.at[where], ops.at[where], sems.at[k]))
    down_loads = [
        pltpu.make_async_copy(source, target, down_sems.at[k])
        for k, (source, target) in enumerate(((dnh_hbm, dnh), (dnl_hbm, dnl)))
    ]
    queue = loads + down_loads

    def begin(count):
        for _ in range(count):
            queue.pop(0).start()

    begin(FIRST[0])
    parents = rows.shape[1] - 8
    rows[:, pl.ds(parents, 8), :] = jnp.zeros((8, 8, n), F32)
    upper[...] = jnp.zeros_like(upper)
    for k in range(3):
        tiles[k] = table[:, pl.ds(128 * k, 128)]
    for q in range(4):
        first, rest, second = [tiles[k, pl.ds(q, parents, stride=4), :] for k in range(3)]
        for i, (body, tail) in enumerate(((first, rest), (second, pltpu.roll(rest, SHIFT, 1)))):
            rows[2 * q + i, pl.ds(0, parents), pl.ds(0, 128)] = body
            rows[2 * q + i, pl.ds(0, parents), pl.ds(128, n - 128)] = tail[:, : n - 128]
    begin(FIRST[1])
    total = None
    for o in range(8):
        both = jnp.concatenate(split(rows[o, pl.ds(0, parents), :]), axis=0)
        term = mm_nt(both, uph[o])
        term = term[:parents] + term[parents:] + mm_nt(both[:parents], upl[o])
        total = term if total is None else total + term
    upper[pl.ds(0, parents), :] = total
    begin(FIRST[2])
    parent = place[0] // 4
    for j in range(slots):
        for t in range(2):
            index = tl[t, j]
            index = jnp.where(index >= 0, index, parents * 8)
            chosen[3 * j + t] = jnp.broadcast_to(rows[index & 7, pl.ds(index >> 3, 1), :], (8, n))
        index = ul[j, parent]
        index = jnp.where(index >= 0, index, parents)
        chosen[3 * j + 2] = jnp.broadcast_to(upper[pl.ds(index, 1), :], (8, n))
    begin(len(queue))

    def block(start, size):
        edges = [(at, min(8, size - at)) for at in range(0, size, 8)]
        sums = [[jnp.zeros((height, n), F32)] * 3 for _, height in edges]
        for j in range(slots):
            factors = [chosen[3 * j + t] for t in range(3)]
            for part, (at, height) in zip(sums, edges, strict=True):
                piece = ops[j, pl.ds(start + at, height), :]
                for t in range(3):
                    part[t] = part[t] + piece * factors[t][:height]
        for part, (at, height) in zip(sums, edges, strict=True):
            s0, s1, s2 = [jnp.sum(s, axis=1, keepdims=True) for s in part]
            lane = lax.broadcasted_iota(I32, (height, 128), 1)
            where = pl.ds(start + at, height)
            top_col[where, :] = jnp.where(lane == 0, s0, jnp.where(lane == 1, s1, 0.0))
            upper_col[where, :] = jnp.where(lane < 2, s2, 0.0)

    def step(i, carry):
        at = pl.multiple_of(i * TALL, TALL)
        where = (slice(None), pl.ds(at, TALL))
        pltpu.make_async_copy(ops_hbm.at[where], ops.at[where], sems.at[i]).wait()
        block(at, TALL)
        return carry

    lax.fori_loop(0, n // TALL, step, 0)
    if n % TALL:
        loads[-1].wait()
        block(n // TALL * TALL, n % TALL)
    for load in down_loads:
        load.wait()
    both = jnp.concatenate(split(upper_col[...]), axis=1)
    octant = lax.rem(place[0] * 2, 8)
    lane = lax.broadcasted_iota(I32, (n, 128), 1)
    from_upper = [halves(mm(dnh[octant + i], both) + mm(dnl[octant + i], both)) for i in range(2)]
    local_top = top_col[...] + jnp.where(lane == 0, from_upper[0], jnp.where(lane == 1, from_upper[1], 0.0))
    local_mid = lowered(local_top, dnh, dnl) + mid_term[...]
    local_mid = jnp.where(lane < 16, local_mid, 0.0)
    local_fine = lowered(local_mid, dnh, dnl) + fine_term[...]
    for i in range(out.shape[0]):
        out[i] = local_fine


def far_terms(place, top_list, upper_list, table, uph, upl, dnh, dnl, fine_term, mid_term, ops, copies):
    slots, n = ops.shape[0], ops.shape[1]
    parents = table.shape[0] // 4
    vm, sm = pl.BlockSpec(memory_space=VMEM), pl.BlockSpec(memory_space=pltpu.SMEM)
    return pl.pallas_call(
        far_kernel,
        out_shape=VMEM((copies, n, 128), F32),
        in_specs=[sm] * 3 + [vm] * 5 + [pl.BlockSpec(memory_space=pltpu.HBM)] * 3,
        out_specs=vm,
        scratch_shapes=[
            pltpu.VMEM((slots, n, n), F32),
            pltpu.VMEM((8, n, n), BF16),
            pltpu.VMEM((8, n, n), BF16),
            pltpu.VMEM((3, table.shape[0], 128), F32),
            pltpu.VMEM((8, parents + 8, n), F32),
            pltpu.VMEM((parents + 8, n), F32),
            pltpu.VMEM((3 * slots, 8, n), F32),
            pltpu.VMEM((n, 128), F32),
            pltpu.VMEM((n, 128), F32),
            pltpu.SemaphoreType.DMA((-(-n // TALL),)),
            pltpu.SemaphoreType.DMA((2,)),
        ],
        compiler_params=pltpu.CompilerParams(vmem_limit_bytes=20 << 20),
        name="far_terms",
    )(
        place, jnp.transpose(top_list), upper_list, table, uph, upl, fine_term, mid_term,
        in_hbm(dnh), in_hbm(dnl), in_hbm(ops),
    )


def exponents():
    entries = []
    for degree in range(ORDER + 1):
        for along_x in range(degree, -1, -1):
            for along_y in range(degree - along_x, -1, -1):
                entries.append((along_x, along_y, degree - along_x - along_y))
    return entries


def monomial_kernel(powers, coords, high_ref, low_ref):
    value = None
    for axis in range(3):
        e = powers[:, pl.ds(axis, 1)]
        base = coords[pl.ds(axis, 1), :]
        for bit in range(4):
            factor = jnp.where((e >> bit) & 1 == 1, base, 1.0)
            value = factor if value is None else value * factor
            base = base * base
    high_ref[...], low_ref[...] = split(value)


def monomials(coords):
    table = jnp.asarray(exponents(), I32)
    n, particles = table.shape[0], coords.shape[1]
    width = 512
    return pl.pallas_call(
        monomial_kernel,
        grid=(particles // width,),
        out_shape=(jax.ShapeDtypeStruct((n, particles), BF16),) * 2,
        in_specs=[pl.BlockSpec((n, 3), lambda i: (0, 0)), pl.BlockSpec((3, width), lambda i: (0, i))],
        out_specs=(pl.BlockSpec((n, width), lambda i: (0, i)),) * 2,
        compiler_params=pltpu.CompilerParams(vmem_limit_bytes=4 << 20),
        name="monomials",
    )(table, coords)


def potential_kernel(place, parts, leaves, high_ref, low_ref, fine_ref, out):
    fine = parts[0] + parts[1] + parts[2] + parts[3]
    fine_ref[...] = fine
    fh, fl = split(jnp.transpose(fine))
    width = 512
    cell = lax.broadcasted_iota(I32, (128, width), 0) + place[0] * 128
    for k in range(out.shape[1] // width):
        at = pl.ds(k * width, width)
        mh, ml = high_ref[:, at], low_ref[:, at]
        values = mm(fh, mh) + mm(fl, mh) + mm(fh, ml)
        out[:, at] = jnp.sum(jnp.where(cell == leaves[:, at], values, 0.0), axis=0, keepdims=True)


def potentials(place, parts, leaves, high, low):
    n = parts.shape[1]
    particles = leaves.shape[1]
    vm = pl.BlockSpec(memory_space=VMEM)
    return pl.pallas_call(
        potential_kernel,
        out_shape=(jax.ShapeDtypeStruct((n, 128), F32), jax.ShapeDtypeStruct((1, particles), F32)),
        in_specs=[pl.BlockSpec(memory_space=pltpu.SMEM)] + [vm] * 4,
        out_specs=(vm,) * 2,
        compiler_params=pltpu.CompilerParams(vmem_limit_bytes=4 << 20),
        name="potentials",
    )(place, parts, leaves, high, low)


DOM = ("dom_0", "dom_1", "dom_2")
DOM_SUB = ("dom_0", "dom_1", "dom_2", "sub")


def exchanged(copies, axes):
    return lax.all_to_all(copies, axes, split_axis=0, concat_axis=0, tiled=True)


def copied(value, count):
    return jnp.broadcast_to(value, (count, *value.shape))


def shards(
    fine_partial,
    upward_ops,
    interaction_ops,
    downward_ops,
    fine_list,
    mid_list,
    top_list,
    upper_list,
    positions,
    leaf_cell,
):
    subs, slabs = lax.axis_size("sub"), lax.axis_size(DOM)
    domain = lax.axis_index(DOM).astype(I32)
    place = domain.reshape(1)
    uph, upl = split_ops(upward_ops)
    dnh, dnl = split_ops(downward_ops, pltpu.HBM)
    parts = exchanged(copied(lax.optimization_barrier(jnp.transpose(fine_partial, (1, 0, 2))), subs), "sub")
    own, tops = own_moments(parts, uph, upl, lax.axis_size(DOM[1:]))
    line = exchanged(tops, DOM[1:])
    left = lax.ppermute(own, DOM, [(i, i + 1) for i in range(slabs - 1)])
    right = lax.ppermute(own, DOM, [(i + 1, i) for i in range(slabs - 1)])
    table = exchanged(line_copies(line, lax.axis_size(DOM[0])), DOM[0])
    table = table.reshape(-1, table.shape[2])
    fine_term, mid_term = near_terms(place, left, own, right, fine_list, mid_list, interaction_ops)
    partial = far_terms(
        place, top_list, upper_list, table, uph, upl, dnh, dnl, fine_term, mid_term, interaction_ops, subs
    )
    high, low = monomials(positions)
    parts = exchanged(partial, "sub")
    local_fine, potential = potentials(place, parts, leaf_cell.reshape(1, -1), high, low)
    return local_fine, potential.reshape(-1)


def solution(mesh):
    torus = Mesh(
        mesh.devices.reshape(8, 12, 2, mesh.shape["sub"]), ("dom_0", "dom_1", "dom_2", "sub")
    )
    return jax.shard_map(
        shards,
        mesh=torus,
        in_specs=(
            P("sub", None, DOM),
            P(),
            P("sub", None, None),
            P(),
            P("sub", DOM),
            P("sub", DOM),
            P("sub", DOM),
            P("sub", None),
            P(None, DOM_SUB),
            P(DOM_SUB),
        ),
        out_specs=(P(None, DOM), P(DOM_SUB)),
        check_vma=False,
    )
```

```python
import jax
import jax.numpy as jnp
from jax import lax
from jax.experimental import pallas as pl
from jax.experimental.pallas import tpu as pltpu
from jax.sharding import Mesh
from jax.sharding import PartitionSpec as P


ORDER = 8
F32, BF16, I32 = jnp.float32, jnp.bfloat16, jnp.int32
VMEM = pltpu.VMEM


def split(value):
    high = value.astype(BF16)
    return high, (value - high.astype(F32)).astype(BF16)


def in_hbm(value):
    return pltpu.with_memory_space_constraint(value, pltpu.HBM)


def halves(pair):
    return pair[:, :128] + pair[:, 128:]


def mm(a, b):
    return jnp.dot(a, b, preferred_element_type=F32)


def mm_nt(a, b):
    return lax.dot_general(a, b, (((1,), (1,)), ((), ())), preferred_element_type=F32)


def gathered(high, low, chosen):
    return jnp.concatenate([mm(high, chosen).astype(BF16), mm(low, chosen).astype(BF16)], axis=1)


def ones_where(shape, test):
    rows = lax.broadcasted_iota(I32, shape, 0)
    lanes = lax.broadcasted_iota(I32, shape, 1)
    return test(rows, lanes).astype(F32).astype(BF16)


def octant_sum(high, low, pair):
    lane = lax.broadcasted_iota(I32, (1, 256), 1) % 8
    total = None
    for o in range(8):
        term = mm(high[o], pair) + mm(low[o], pair)
        total = jnp.where(lane == o, term, 0.0 if total is None else total)
    return halves(total)


def raised(moments, uph, upl):
    summed = octant_sum(uph, upl, jnp.concatenate(split(moments), axis=1))
    parent = ones_where((128, 128), lambda r, c: r // 8 == c)
    high, low = split(summed)
    return mm(high, parent) + mm(low, parent)


def lowered(expansion, dnh, dnl):
    child = ones_where((128, 128), lambda r, c: c // 8 == r)
    return octant_sum(dnh, dnl, gathered(*split(expansion), child))


PITCH = 56


def split_kernel(ops_hbm, *refs):
    count = (len(refs) - 4) // 2
    small, (high, low), kept, (parts, sems) = refs[:count], refs[count : count + 2], refs[count + 2 : -2], refs[-2:]
    copies = [pltpu.make_async_copy(ops_hbm.at[:, o, :], parts.at[o], sems.at[o]) for o in range(8)]
    for copy in copies:
        copy.start()
    if small:
        top = small[0][...]
        kept[0][...] = jnp.where(top >= 0, (top & 7) * PITCH + (top >> 3), PITCH - 8)
        upper = small[1][...]
        kept[1][...] = jnp.where(upper >= 0, upper, PITCH - 8)
    for source, target in zip(small[2:], kept[2:], strict=True):
        target[...] = source[...]
    for o in range(8):
        copies[o].wait()
        high[o], low[o] = split(parts[o])


def split_ops(ops, kept=VMEM, small=()):
    n = ops.shape[1]
    vm = pl.BlockSpec(memory_space=VMEM)
    return pl.pallas_call(
        split_kernel,
        out_shape=(kept((8, n, n), BF16),) * 2 + tuple(VMEM(x.shape, x.dtype) for x in small),
        in_specs=[pl.BlockSpec(memory_space=pltpu.HBM)] + [vm] * len(small),
        out_specs=(vm,) * (2 + len(small)),
        scratch_shapes=[pltpu.VMEM((8, n, n), F32), pltpu.SemaphoreType.DMA((8,))],
        compiler_params=pltpu.CompilerParams(vmem_limit_bytes=8 << 20),
    )(in_hbm(jnp.transpose(ops, (1, 0, 2))), *(in_hbm(x) for x in small))


def copies_kernel(part_hbm, out_hbm, buffer, sems):
    load = pltpu.make_async_copy(part_hbm, buffer, sems.at[0])
    load.start()
    load.wait()
    stores = [pltpu.make_async_copy(buffer, out_hbm.at[i], sems.at[i + 1]) for i in range(out_hbm.shape[0])]
    for store in stores:
        store.start()
    for store in stores:
        store.wait()


def part_copies(part, copies):
    hbm = pl.BlockSpec(memory_space=pltpu.HBM)
    return pl.pallas_call(
        copies_kernel,
        out_shape=pltpu.HBM((copies, *part.shape), F32),
        in_specs=[hbm],
        out_specs=hbm,
        scratch_shapes=[pltpu.VMEM(part.shape, F32), pltpu.SemaphoreType.DMA((copies + 1,))],
        compiler_params=pltpu.CompilerParams(vmem_limit_bytes=2 << 20),
        name="part_copies",
    )(in_hbm(part))


MID_AT = 168
SHIFT = 64


def packed(first, second):
    n = first.shape[1]
    blank = jnp.zeros((1, SHIFT - (n - 128)), F32)
    rests = jnp.concatenate([first[:, 128:], blank, second[:, 128:], blank], axis=1)
    return jnp.concatenate([first[:, :128], rests, second[:, :128]], axis=1)


def own_kernel(parts, uph, upl, own_ref, top_ref):
    n = parts.shape[1]
    fine = (parts[0] + parts[1] + parts[2] + parts[3])[:, 0, :]
    own_ref[pl.ds(0, n), :] = fine
    mid = raised(fine, uph, upl)
    rows = jnp.transpose(mid)[:16]
    own_ref[pl.ds(MID_AT, 16), :] = rows[:, :128]
    own_ref[pl.ds(MID_AT + 16, 16), pl.ds(0, n - 128)] = rows[:, 128:]
    rows = jnp.transpose(raised(mid, uph, upl))
    row = packed(rows[:1], rows[1:2])
    for i in range(top_ref.shape[0]):
        top_ref[i] = row


def own_moments(parts, uph, upl, copies):
    return pl.pallas_call(
        own_kernel,
        out_shape=(VMEM((MID_AT + 32, 128), F32), VMEM((copies, 1, 384), F32)),
        in_specs=[pl.BlockSpec(memory_space=VMEM)] * 3,
        out_specs=(pl.BlockSpec(memory_space=VMEM),) * 2,
        compiler_params=pltpu.CompilerParams(vmem_limit_bytes=4 << 20),
        name="own_moments",
    )(parts, uph, upl)


def line_kernel(line, out):
    rows = jnp.concatenate([line[r ^ 1] for r in range(line.shape[0] - 1, -1, -1)], axis=0)
    for i in range(out.shape[0]):
        out[i] = rows


def line_copies(line, copies):
    return pl.pallas_call(
        line_kernel,
        out_shape=jax.ShapeDtypeStruct((copies, line.shape[0], line.shape[2]), F32),
        in_specs=[pl.BlockSpec(memory_space=VMEM)],
        out_specs=pl.BlockSpec(memory_space=VMEM),
        compiler_params=pltpu.CompilerParams(vmem_limit_bytes=2 << 20),
        name="line_copies",
    )(line)


GROUP = 4


def near_kernel(place, outer, own, partner, fl, ml, ops_hbm, fine_out, mid_out, ops, full, rows, mids, mid_rows, xa, xb, acc_a, acc_b, sems):
    slots, n = ops.shape[0], ops.shape[1]
    groups = -(-slots // GROUP)
    size = [min(GROUP, slots - k * GROUP) for k in range(groups)]
    copies = []
    for k in range(0, groups, 2):
        at = pl.ds(k * GROUP, sum(size[k : k + 2]))
        copies.append(pltpu.make_async_copy(ops_hbm.at[at], ops.at[at], sems.at[k // 2]))
        copies[-1].start()
    rows[...] = jnp.zeros_like(rows)
    second = lax.rem(place[0], 2)
    for i, ref in ((2 * second, outer), (1, own), (2 - 2 * second, partner)):
        at = pl.ds(pl.multiple_of(16 * i, 16), 16)
        full[i] = ref[pl.ds(0, n), :]
        rows[at, pl.ds(0, 128)] = ref[pl.ds(MID_AT, 16), :]
        rows[at, pl.ds(128, n - 128)] = ref[pl.ds(MID_AT + 16, 16), pl.ds(0, n - 128)]
    mid = jnp.transpose(rows[...])[:n]
    mids[:, pl.ds(0, 128)], mids[:, pl.ds(128, 128)] = split(mid)
    anchor = place[0] * 128 - 128
    mid_anchor = place[0] * 16 - 16
    lane = lax.broadcasted_iota(I32, (1, 128), 1)
    part = (lane // 16) % 2 * 128
    listed = ml[...]
    listed = jnp.where(listed >= 0, listed - mid_anchor, -1).astype(F32).astype(BF16)
    spread = ones_where((16, 128), lambda r, c: c % 16 == r)
    mid_rows[...] = lax.dot_general(listed, spread, (((0,), (0,)), ((), ())), preferred_element_type=F32).astype(I32)
    acc_a[...] = jnp.zeros_like(acc_a)
    acc_b[...] = jnp.zeros_like(acc_b)

    def load(k, count, xs):
        row = jnp.full((1, 128), -1, I32)
        for jj in range(count):
            row = jnp.where(lane // 32 == jj, mid_rows[pl.ds(k * GROUP + jj, 1), :], row)
        row = jnp.where(row >= 0, row + part, -1)
        source = lax.broadcasted_iota(I32, (256, 128), 0)
        tile = mm(mids[...], (source == row).astype(F32).astype(BF16)).astype(BF16)
        for jj in range(count):
            xs[jj, :, pl.ds(128, 128)] = jnp.where(lane // 32 == jj, tile, jnp.zeros_like(tile))
            row = fl[pl.ds(k * GROUP + jj, 1), :]
            row = jnp.where(row >= 0, row - anchor, 512)
            index = jnp.broadcast_to(row & 127, (n, 128))
            got = jnp.zeros((n, 128), F32)
            for i in range(3):
                moved = jnp.take_along_axis(full[i], index, axis=1, mode="promise_in_bounds")
                got = jnp.where(row >> 7 == i, moved, got)
            xs[jj, :, pl.ds(0, 128)], xs[jj, :, pl.ds(256, 128)] = split(got)

    def use(k, count, xs):
        a = b = None
        for jj in range(count):
            oh, ol = split(ops[k * GROUP + jj])
            x = xs[jj]
            ta = mm(oh, x[:, :256]) + mm(ol, x[:, :256])
            tb = mm(oh, x[:, 256:])
            a = ta if a is None else a + ta
            b = tb if b is None else b + tb
        acc_a[...] += a
        acc_b[...] += b

    load(0, GROUP, xa)

    def ready(i):
        at = pl.ds(0, 2 * GROUP)
        if isinstance(i, int):
            copies[i].wait()
        else:
            pltpu.make_async_copy(ops_hbm.at[at], ops.at[at], sems.at[i]).wait()

    def step(i, carry):
        ready(i)
        load(2 * i + 1, GROUP, xb)
        use(2 * i, GROUP, xa)
        load(2 * i + 2, GROUP, xa)
        use(2 * i + 1, GROUP, xb)
        return carry

    steady = groups // 2 - 1
    lax.fori_loop(0, steady, step, 0)
    bufs = (xa, xb)
    for k in range(2 * steady, groups):
        if k % 2 == 0:
            ready(k // 2)
        if k + 1 < groups:
            load(k + 1, size[k + 1], bufs[(k + 1) % 2])
        use(k, size[k], bufs[k % 2])
    fine_out[...] = acc_a[:, pl.ds(0, 128)] + acc_b[...]
    folded = acc_a[:, pl.ds(128, 128)]
    for shift in (64, 32, 16):
        folded = folded + pltpu.roll(folded, shift, 1)
    mid_out[...] = folded


def near_terms(place, outer, own, partner, fine_list, mid_list, ops):
    slots, n = ops.shape[0], ops.shape[1]
    vm = pl.BlockSpec(memory_space=VMEM)
    return pl.pallas_call(
        near_kernel,
        out_shape=(VMEM((n, 128), F32),) * 2,
        in_specs=[pl.BlockSpec(memory_space=pltpu.SMEM)] + [vm] * 5 + [pl.BlockSpec(memory_space=pltpu.HBM)],
        out_specs=(vm,) * 2,
        scratch_shapes=[
            pltpu.VMEM((slots, n, n), F32),
            pltpu.VMEM((3, n, 128), F32),
            pltpu.VMEM((128, 256), F32),
            pltpu.VMEM((n, 256), BF16),
            pltpu.VMEM((slots, 128), I32),
            pltpu.VMEM((GROUP, n, 384), BF16),
            pltpu.VMEM((GROUP, n, 384), BF16),
            pltpu.VMEM((n, 256), F32),
            pltpu.VMEM((n, 128), F32),
            pltpu.SemaphoreType.DMA((-(-slots // (2 * GROUP)),)),
        ],
        compiler_params=pltpu.CompilerParams(vmem_limit_bytes=20 << 20),
        name="near_terms",
    )(place, outer, own, partner, fine_list, mid_list, in_hbm(ops))


TALL = 24
UNROLL = 8
FIRST = (3, 2, 2)


def far_kernel(
    place, tl_ref, ul_ref, table, uph, upl, fine_term, mid_term, dnh_hbm, dnl_hbm, ops_hbm, out,
    ops, dnh, dnl, tiles, rows, upper, chosen, top_col, upper_col, tl, ul, sems, down_sems, list_sems,
):
    slots, n = ops.shape[0], ops.shape[1]
    lists = [
        pltpu.make_async_copy(source, target, list_sems.at[k])
        for k, (source, target) in enumerate(((tl_ref, tl), (ul_ref, ul)))
    ]
    for copy in lists:
        copy.start()
    loads = []
    for k, at in enumerate(range(0, n, TALL)):
        where = (slice(None), pl.ds(at, min(TALL, n - at)))
        loads.append(pltpu.make_async_copy(ops_hbm.at[where], ops.at[where], sems.at[k]))
    down_loads = [
        pltpu.make_async_copy(source, target, down_sems.at[k])
        for k, (source, target) in enumerate(((dnh_hbm, dnh), (dnl_hbm, dnl)))
    ]
    queue = loads + down_loads

    def begin(count):
        for _ in range(count):
            queue.pop(0).start()

    begin(FIRST[0])
    parents = PITCH - 8
    rows[pl.ds(parents, 8), :] = jnp.zeros((8, n), F32)
    upper[...] = jnp.zeros_like(upper)
    lines = table.shape[0] // 24
    for k in range(3):
        for i in range(lines):
            tiles[k, pl.ds(24 * (lines - 1 - i), 24), :] = table[pl.ds(24 * i, 24), pl.ds(128 * k, 128)]
    for q in range(4):
        first, rest, second = [tiles[k, pl.ds(q, parents, stride=4), :] for k in range(3)]
        for i, (body, tail) in enumerate(((first, rest), (second, pltpu.roll(rest, SHIFT, 1)))):
            at = pl.ds((2 * q + i) * PITCH, parents)
            rows[at, pl.ds(0, 128)] = body
            rows[at, pl.ds(128, n - 128)] = tail[:, : n - 128]
    begin(FIRST[1])
    total = None
    for o in range(8):
        both = jnp.concatenate(split(rows[pl.ds(o * PITCH, parents), :]), axis=0)
        term = mm_nt(both, uph[o])
        term = term[:parents] + term[parents:] + mm_nt(both[:parents], upl[o])
        total = term if total is None else total + term
    upper[pl.ds(0, parents), :] = total
    begin(FIRST[2])
    parent = place[0] // 4
    for copy in lists:
        copy.wait()

    def choose(j):
        for t in range(2):
            chosen[3 * j + t] = jnp.broadcast_to(rows[pl.ds(tl[t, j], 1), :], (8, n))
        chosen[3 * j + 2] = jnp.broadcast_to(upper[pl.ds(ul[j, parent], 1), :], (8, n))

    def some(i, carry):
        for k in range(UNROLL):
            choose(i * UNROLL + k)
        return carry

    lax.fori_loop(0, slots // UNROLL, some, 0)
    for j in range(slots // UNROLL * UNROLL, slots):
        choose(j)
    begin(len(queue))

    def block(start, size):
        edges = [(at, min(8, size - at)) for at in range(0, size, 8)]
        sums = [[jnp.zeros((height, n), F32)] * 3 for _, height in edges]
        for j in range(slots):
            factors = [chosen[3 * j + t] for t in range(3)]
            for part, (at, height) in zip(sums, edges, strict=True):
                piece = ops[j, pl.ds(start + at, height), :]
                for t in range(3):
                    part[t] = part[t] + piece * factors[t][:height]
        for part, (at, height) in zip(sums, edges, strict=True):
            s0, s1, s2 = [jnp.sum(s, axis=1, keepdims=True) for s in part]
            lane = lax.broadcasted_iota(I32, (height, 128), 1)
            where = pl.ds(start + at, height)
            top_col[where, :] = jnp.where(lane == 0, s0, jnp.where(lane == 1, s1, 0.0))
            upper_col[where, :] = jnp.where(lane < 2, s2, 0.0)

    def step(i, carry):
        at = pl.multiple_of(i * TALL, TALL)
        where = (slice(None), pl.ds(at, TALL))
        pltpu.make_async_copy(ops_hbm.at[where], ops.at[where], sems.at[i]).wait()
        block(at, TALL)
        return carry

    lax.fori_loop(0, n // TALL, step, 0)
    if n % TALL:
        loads[-1].wait()
        block(n // TALL * TALL, n % TALL)
    for load in down_loads:
        load.wait()
    both = jnp.concatenate(split(upper_col[...]), axis=1)
    octant = lax.rem(place[0] * 2, 8)
    lane = lax.broadcasted_iota(I32, (n, 128), 1)
    from_upper = [halves(mm(dnh[octant + i], both) + mm(dnl[octant + i], both)) for i in range(2)]
    local_top = top_col[...] + jnp.where(lane == 0, from_upper[0], jnp.where(lane == 1, from_upper[1], 0.0))
    local_mid = lowered(local_top, dnh, dnl) + mid_term[...]
    local_mid = jnp.where(lane < 16, local_mid, 0.0)
    local_fine = lowered(local_mid, dnh, dnl) + fine_term[...]
    for i in range(out.shape[0]):
        out[i] = local_fine


def far_terms(place, top_list, upper_list, table, uph, upl, dnh, dnl, fine_term, mid_term, ops, copies):
    slots, n = ops.shape[0], ops.shape[1]
    parents = table.shape[0] // 4
    vm, sm = pl.BlockSpec(memory_space=VMEM), pl.BlockSpec(memory_space=pltpu.SMEM)
    return pl.pallas_call(
        far_kernel,
        out_shape=VMEM((copies, n, 128), F32),
        in_specs=[sm] + [vm] * 7 + [pl.BlockSpec(memory_space=pltpu.HBM)] * 3,
        out_specs=vm,
        scratch_shapes=[
            pltpu.VMEM((slots, n, n), F32),
            pltpu.VMEM((8, n, n), BF16),
            pltpu.VMEM((8, n, n), BF16),
            pltpu.VMEM((3, table.shape[0], 128), F32),
            pltpu.VMEM((8 * PITCH, n), F32),
            pltpu.VMEM((parents + 8, n), F32),
            pltpu.VMEM((3 * slots, 8, n), F32),
            pltpu.VMEM((n, 128), F32),
            pltpu.VMEM((n, 128), F32),
            pltpu.SMEM(top_list.shape, I32),
            pltpu.SMEM(upper_list.shape, I32),
            pltpu.SemaphoreType.DMA((-(-n // TALL),)),
            pltpu.SemaphoreType.DMA((2,)),
            pltpu.SemaphoreType.DMA((2,)),
        ],
        compiler_params=pltpu.CompilerParams(vmem_limit_bytes=20 << 20),
        name="far_terms",
    )(
        place, top_list, upper_list, table, uph, upl, fine_term, mid_term,
        in_hbm(dnh), in_hbm(dnl), in_hbm(ops),
    )


def exponents():
    entries = []
    for degree in range(ORDER + 1):
        for along_x in range(degree, -1, -1):
            for along_y in range(degree - along_x, -1, -1):
                entries.append((along_x, along_y, degree - along_x - along_y))
    return entries


def monomial_kernel(powers, coords, high_ref, low_ref):
    value = None
    for axis in range(3):
        e = powers[:, pl.ds(axis, 1)]
        base = coords[pl.ds(axis, 1), :]
        for bit in range(4):
            factor = jnp.where((e >> bit) & 1 == 1, base, 1.0)
            value = factor if value is None else value * factor
            base = base * base
    high_ref[...], low_ref[...] = split(value)


def monomials(coords):
    table = jnp.asarray(exponents(), I32)
    n, particles = table.shape[0], coords.shape[1]
    width = 512
    return pl.pallas_call(
        monomial_kernel,
        grid=(particles // width,),
        out_shape=(pltpu.HBM((n, particles), BF16),) * 2,
        in_specs=[pl.BlockSpec((n, 3), lambda i: (0, 0)), pl.BlockSpec((3, width), lambda i: (0, i))],
        out_specs=(pl.BlockSpec((n, width), lambda i: (0, i)),) * 2,
        compiler_params=pltpu.CompilerParams(vmem_limit_bytes=4 << 20),
        name="monomials",
    )(table, coords)


def potential_kernel(place, parts, leaves, high_ref, low_ref, fine_ref, out):
    fine = parts[0] + parts[1] + parts[2] + parts[3]
    fine_ref[...] = fine
    fh, fl = split(jnp.transpose(fine))
    width = 512
    cell = lax.broadcasted_iota(I32, (128, width), 0) + place[0] * 128
    for k in range(out.shape[1] // width):
        at = pl.ds(k * width, width)
        mh, ml = high_ref[:, at], low_ref[:, at]
        values = mm(fh, mh) + mm(fl, mh) + mm(fh, ml)
        out[:, at] = jnp.sum(jnp.where(cell == leaves[:, at], values, 0.0), axis=0, keepdims=True)


def potentials(place, parts, leaves, high, low):
    n = parts.shape[1]
    particles = leaves.shape[1]
    vm = pl.BlockSpec(memory_space=VMEM)
    return pl.pallas_call(
        potential_kernel,
        out_shape=(jax.ShapeDtypeStruct((n, 128), F32), jax.ShapeDtypeStruct((1, particles), F32)),
        in_specs=[pl.BlockSpec(memory_space=pltpu.SMEM)] + [vm] * 4,
        out_specs=(vm,) * 2,
        compiler_params=pltpu.CompilerParams(vmem_limit_bytes=4 << 20),
        name="potentials",
    )(place, parts, leaves, high, low)


DOM = ("dom_0", "dom_1")
DOM_SUB = ("dom_0", "dom_1", "sub")


ORDER_1 = [i ^ 1 for i in range(23, -1, -1)]
ORDER_0 = list(range(7, -1, -1))


def exchanged(copies, axis, order=None):
    groups = None if order is None else [order]
    return lax.all_to_all(copies, axis, split_axis=0, concat_axis=0, tiled=True, axis_index_groups=groups)


def shards(
    fine_partial,
    upward_ops,
    interaction_ops,
    downward_ops,
    fine_list,
    mid_list,
    top_list,
    upper_list,
    positions,
    leaf_cell,
):
    subs, slabs = lax.axis_size("sub"), lax.axis_size(DOM)
    domain = lax.axis_index(DOM).astype(I32)
    place = domain.reshape(1)
    lists = (jnp.transpose(top_list), upper_list, fine_list, jnp.transpose(mid_list))
    uph, upl, top_list, upper_list, fine_list, mid_list = split_ops(upward_ops, small=lists)
    dnh, dnl = split_ops(downward_ops, pltpu.HBM)
    parts = exchanged(part_copies(jnp.transpose(fine_partial, (1, 0, 2)), subs), "sub")
    own, tops = own_moments(parts, uph, upl, lax.axis_size(DOM[1]))
    line = exchanged(tops, DOM[1], ORDER_1)
    outer = lax.ppermute(own, DOM, [(i, i + 2 * (i % 2) - 1) for i in range(1, slabs - 1)])
    partner = lax.ppermute(own, DOM, [(i, i ^ 1) for i in range(slabs)])
    table = exchanged(line_copies(line, lax.axis_size(DOM[0])), DOM[0], ORDER_0)
    table = table.reshape(-1, table.shape[2])
    fine_term, mid_term = near_terms(place, outer, own, partner, fine_list, mid_list, interaction_ops)
    partial = far_terms(
        place, top_list, upper_list, table, uph, upl, dnh, dnl, fine_term, mid_term, interaction_ops, subs
    )
    high, low = monomials(positions)
    parts = exchanged(partial, "sub")
    local_fine, potential = potentials(place, parts, leaf_cell.reshape(1, -1), high, low)
    return local_fine, potential.reshape(-1)


def solution(mesh):
    torus = Mesh(
        mesh.devices.reshape(8, 24, mesh.shape["sub"]), ("dom_0", "dom_1", "sub")
    )
    return jax.shard_map(
        shards,
        mesh=torus,
        in_specs=(
            P("sub", None, DOM),
            P(),
            P("sub", None, None),
            P(),
            P("sub", DOM),
            P("sub", DOM),
            P("sub", DOM),
            P("sub", None),
            P(None, DOM_SUB),
            P(DOM_SUB),
        ),
        out_specs=(P(None, DOM), P(DOM_SUB)),
        check_vma=False,
    )
```

```python
import jax
import jax.numpy as jnp
from jax import lax
from jax.experimental import pallas as pl
from jax.experimental.pallas import tpu as pltpu
from jax.sharding import Mesh
from jax.sharding import PartitionSpec as P


ORDER = 8
F32, BF16, I32 = jnp.float32, jnp.bfloat16, jnp.int32
VMEM = pltpu.VMEM
ORDER_0 = [6, 7, 5, 4, 3, 2, 1, 0]
ORDER_1 = list(range(23, -1, -1))


def split(value):
    high = value.astype(BF16)
    return high, (value - high.astype(F32)).astype(BF16)


def in_hbm(value):
    return pltpu.with_memory_space_constraint(value, pltpu.HBM)


def halves(pair):
    return pair[:, :128] + pair[:, 128:]


def mm(a, b):
    return jnp.dot(a, b, preferred_element_type=F32)


def mm_nt(a, b):
    return lax.dot_general(a, b, (((1,), (1,)), ((), ())), preferred_element_type=F32)


def gathered(high, low, chosen):
    return jnp.concatenate([mm(high, chosen).astype(BF16), mm(low, chosen).astype(BF16)], axis=1)


def ones_where(shape, test):
    rows = lax.broadcasted_iota(I32, shape, 0)
    lanes = lax.broadcasted_iota(I32, shape, 1)
    return test(rows, lanes).astype(F32).astype(BF16)


def octant_sum(high, low, pair):
    lane = lax.broadcasted_iota(I32, (1, 256), 1) % 8
    total = None
    for o in range(8):
        term = mm(high[o], pair) + mm(low[o], pair)
        total = jnp.where(lane == o, term, 0.0 if total is None else total)
    return halves(total)


def raised(moments, uph, upl):
    summed = octant_sum(uph, upl, jnp.concatenate(split(moments), axis=1))
    parent = ones_where((128, 128), lambda r, c: r // 8 == c)
    high, low = split(summed)
    return mm(high, parent) + mm(low, parent)


def lowered(expansion, dnh, dnl):
    child = ones_where((128, 128), lambda r, c: c // 8 == r)
    return octant_sum(dnh, dnl, gathered(*split(expansion), child))


PITCH = 56


def split_kernel(ops_hbm, *refs):
    count = (len(refs) - 2) // 2 if len(refs) > 4 else 0
    small, (high, low), kept, (parts, sems) = refs[:count], refs[count : count + 2], refs[count + 2 : -2], refs[-2:]
    copies = [pltpu.make_async_copy(ops_hbm.at[:, o, :], parts.at[o], sems.at[o]) for o in range(8)]
    for copy in copies:
        copy.start()
    if small:
        place, top_ref, upper_ref, *others = small
        top = top_ref[...]
        kept[0][pl.ds(0, 2), :] = jnp.where(top >= 0, (top & 7) * PITCH + (top >> 3), PITCH - 8)
        upper = upper_ref[...]
        upper = jnp.where(upper >= 0, upper, PITCH - 8).astype(F32).astype(BF16)
        here = ones_where((8, upper.shape[1]), lambda r, c: c == place[0] // 4)
        kept[0][pl.ds(2, 1), :] = mm_nt(here, upper)[:1].astype(I32)
        for source, target in zip(others, kept[1:], strict=True):
            target[...] = source[...]
    for o in range(8):
        copies[o].wait()
        high[o], low[o] = split(parts[o])


def split_ops(ops, kept=VMEM, lists=()):
    n = ops.shape[1]
    vm, sm = pl.BlockSpec(memory_space=VMEM), pl.BlockSpec(memory_space=pltpu.SMEM)
    more = (VMEM((3, lists[1].shape[1]), I32), *(VMEM(x.shape, I32) for x in lists[3:])) if lists else ()
    return pl.pallas_call(
        split_kernel,
        out_shape=(kept((8, n, n), BF16),) * 2 + more,
        in_specs=[pl.BlockSpec(memory_space=pltpu.HBM)] + [sm] * bool(lists) + [vm] * (len(lists) - 1),
        out_specs=(vm,) * (2 + len(more)),
        scratch_shapes=[pltpu.VMEM((8, n, n), F32), pltpu.SemaphoreType.DMA((8,))],
        compiler_params=pltpu.CompilerParams(vmem_limit_bytes=8 << 20),
    )(in_hbm(jnp.transpose(ops, (1, 0, 2))), *lists[:1], *(in_hbm(x) for x in lists[1:]))


def copies_kernel(part_hbm, out_hbm, buffer, sems):
    load = pltpu.make_async_copy(part_hbm, buffer, sems.at[0])
    load.start()
    load.wait()
    stores = [pltpu.make_async_copy(buffer, out_hbm.at[i], sems.at[i + 1]) for i in range(out_hbm.shape[0])]
    for store in stores:
        store.start()
    for store in stores:
        store.wait()


def part_copies(part, copies):
    hbm = pl.BlockSpec(memory_space=pltpu.HBM)
    return pl.pallas_call(
        copies_kernel,
        out_shape=pltpu.HBM((copies, *part.shape), F32),
        in_specs=[hbm],
        out_specs=hbm,
        scratch_shapes=[pltpu.VMEM(part.shape, F32), pltpu.SemaphoreType.DMA((copies + 1,))],
        compiler_params=pltpu.CompilerParams(vmem_limit_bytes=2 << 20),
        name="part_copies",
    )(in_hbm(part))


MID_AT = 168
SHIFT = 64
TAIL = 37
LINE_ROWS = 64


def packed(first, second):
    n = first.shape[1]
    blank = jnp.zeros((1, SHIFT - (n - 128)), F32)
    rests = jnp.concatenate([first[:, 128:], blank, second[:, 128:], blank], axis=1)
    return jnp.concatenate([first[:, :128], rests, second[:, :128]], axis=1)


def own_kernel(parts, uph, upl, own_ref, top_ref):
    n = parts.shape[1]
    fine = (parts[0] + parts[1] + parts[2] + parts[3])[:, 0, :]
    own_ref[pl.ds(0, n), :] = fine
    mid = raised(fine, uph, upl)
    rows = jnp.transpose(mid)[:16]
    own_ref[pl.ds(MID_AT, 16), :] = rows[:, :128]
    own_ref[pl.ds(MID_AT + 16, 16), pl.ds(0, n - 128)] = rows[:, 128:]
    rows = jnp.transpose(raised(mid, uph, upl))
    row = packed(rows[:1], rows[1:2])
    for i in range(top_ref.shape[0]):
        top_ref[i] = row


def own_moments(parts, uph, upl, copies):
    return pl.pallas_call(
        own_kernel,
        out_shape=(VMEM((MID_AT + 32, 128), F32), VMEM((copies, 1, 384), F32)),
        in_specs=[pl.BlockSpec(memory_space=VMEM)] * 3,
        out_specs=(pl.BlockSpec(memory_space=VMEM),) * 2,
        compiler_params=pltpu.CompilerParams(vmem_limit_bytes=4 << 20),
        name="own_moments",
    )(parts, uph, upl)


def line_kernel(line, out):
    rows = jnp.concatenate([line[ORDER_1.index(i)] for i in range(line.shape[0])], axis=0)
    first, second, third = [rows[8 * g : 8 * g + 8, 128:256] for g in range(3)]
    lane = lax.broadcasted_iota(I32, (8, 128), 1)

    def beside(one, two, three):
        return jnp.where(lane < TAIL, one, jnp.where(lane < 2 * TAIL, two, three))

    tails = (
        beside(first, pltpu.roll(first, 128 + TAIL - SHIFT, 1), pltpu.roll(second, 2 * TAIL, 1)),
        beside(pltpu.roll(second, SHIFT, 1), pltpu.roll(third, TAIL, 1), pltpu.roll(third, 2 * TAIL - SHIFT, 1)),
    )
    packed_rows = jnp.concatenate([rows[:, :128], rows[:, 256:], *tails], axis=0)
    for i in range(out.shape[0]):
        out[i] = packed_rows


def line_copies(line, copies):
    return pl.pallas_call(
        line_kernel,
        out_shape=jax.ShapeDtypeStruct((copies, LINE_ROWS, 128), F32),
        in_specs=[pl.BlockSpec(memory_space=VMEM)],
        out_specs=pl.BlockSpec(memory_space=VMEM),
        compiler_params=pltpu.CompilerParams(vmem_limit_bytes=2 << 20),
        name="line_copies",
    )(line)


GROUP = 4


def near_kernel(place, outer, own, partner, fl, ml, ops_hbm, fine_out, mid_out, ops, full, rows, mids, mid_rows, xa, xb, acc_a, acc_b, sems):
    slots, n = ops.shape[0], ops.shape[1]
    groups = -(-slots // GROUP)
    size = [min(GROUP, slots - k * GROUP) for k in range(groups)]
    copies = []
    for k in range(0, groups, 2):
        at = pl.ds(k * GROUP, sum(size[k : k + 2]))
        copies.append(pltpu.make_async_copy(ops_hbm.at[at], ops.at[at], sems.at[k // 2]))
        copies[-1].start()
    rows[...] = jnp.zeros_like(rows)
    second = lax.rem(place[0], 2)
    for i, ref in ((2 * second, outer), (1, own), (2 - 2 * second, partner)):
        at = pl.ds(pl.multiple_of(16 * i, 16), 16)
        full[i] = ref[pl.ds(0, n), :]
        rows[at, pl.ds(0, 128)] = ref[pl.ds(MID_AT, 16), :]
        rows[at, pl.ds(128, n - 128)] = ref[pl.ds(MID_AT + 16, 16), pl.ds(0, n - 128)]
    mid = jnp.transpose(rows[...])[:n]
    mids[:, pl.ds(0, 128)], mids[:, pl.ds(128, 128)] = split(mid)
    anchor = place[0] * 128 - 128
    mid_anchor = place[0] * 16 - 16
    lane = lax.broadcasted_iota(I32, (1, 128), 1)
    part = (lane // 16) % 2 * 128
    listed = ml[...]
    listed = jnp.where(listed >= 0, listed - mid_anchor, -1).astype(F32).astype(BF16)
    spread = ones_where((16, 128), lambda r, c: c % 16 == r)
    mid_rows[...] = lax.dot_general(listed, spread, (((0,), (0,)), ((), ())), preferred_element_type=F32).astype(I32)
    acc_a[...] = jnp.zeros_like(acc_a)
    acc_b[...] = jnp.zeros_like(acc_b)

    def load(k, count, xs):
        row = jnp.full((1, 128), -1, I32)
        for jj in range(count):
            row = jnp.where(lane // 32 == jj, mid_rows[pl.ds(k * GROUP + jj, 1), :], row)
        row = jnp.where(row >= 0, row + part, -1)
        source = lax.broadcasted_iota(I32, (256, 128), 0)
        tile = mm(mids[...], (source == row).astype(F32).astype(BF16)).astype(BF16)
        for jj in range(count):
            xs[jj, :, pl.ds(128, 128)] = jnp.where(lane // 32 == jj, tile, jnp.zeros_like(tile))
            row = fl[pl.ds(k * GROUP + jj, 1), :]
            row = jnp.where(row >= 0, row - anchor, 512)
            index = jnp.broadcast_to(row & 127, (n, 128))
            got = jnp.zeros((n, 128), F32)
            for i in range(3):
                moved = jnp.take_along_axis(full[i], index, axis=1, mode="promise_in_bounds")
                got = jnp.where(row >> 7 == i, moved, got)
            xs[jj, :, pl.ds(0, 128)], xs[jj, :, pl.ds(256, 128)] = split(got)

    def use(k, count, xs):
        a = b = None
        for jj in range(count):
            oh, ol = split(ops[k * GROUP + jj])
            x = xs[jj]
            ta = mm(oh, x[:, :256]) + mm(ol, x[:, :256])
            tb = mm(oh, x[:, 256:])
            a = ta if a is None else a + ta
            b = tb if b is None else b + tb
        acc_a[...] += a
        acc_b[...] += b

    load(0, GROUP, xa)

    def ready(i):
        at = pl.ds(0, 2 * GROUP)
        if isinstance(i, int):
            copies[i].wait()
        else:
            pltpu.make_async_copy(ops_hbm.at[at], ops.at[at], sems.at[i]).wait()

    def step(i, carry):
        ready(i)
        load(2 * i + 1, GROUP, xb)
        use(2 * i, GROUP, xa)
        load(2 * i + 2, GROUP, xa)
        use(2 * i + 1, GROUP, xb)
        return carry

    steady = groups // 2 - 1
    lax.fori_loop(0, steady, step, 0)
    bufs = (xa, xb)
    for k in range(2 * steady, groups):
        if k % 2 == 0:
            ready(k // 2)
        if k + 1 < groups:
            load(k + 1, size[k + 1], bufs[(k + 1) % 2])
        use(k, size[k], bufs[k % 2])
    fine_out[...] = acc_a[:, pl.ds(0, 128)] + acc_b[...]
    folded = acc_a[:, pl.ds(128, 128)]
    for shift in (64, 32, 16):
        folded = folded + pltpu.roll(folded, shift, 1)
    mid_out[...] = folded


def near_terms(place, outer, own, partner, fine_list, mid_list, ops):
    slots, n = ops.shape[0], ops.shape[1]
    vm = pl.BlockSpec(memory_space=VMEM)
    return pl.pallas_call(
        near_kernel,
        out_shape=(VMEM((n, 128), F32),) * 2,
        in_specs=[pl.BlockSpec(memory_space=pltpu.SMEM)] + [vm] * 5 + [pl.BlockSpec(memory_space=pltpu.HBM)],
        out_specs=(vm,) * 2,
        scratch_shapes=[
            pltpu.VMEM((slots, n, n), F32),
            pltpu.VMEM((3, n, 128), F32),
            pltpu.VMEM((128, 256), F32),
            pltpu.VMEM((n, 256), BF16),
            pltpu.VMEM((slots, 128), I32),
            pltpu.VMEM((GROUP, n, 384), BF16),
            pltpu.VMEM((GROUP, n, 384), BF16),
            pltpu.VMEM((n, 256), F32),
            pltpu.VMEM((n, 128), F32),
            pltpu.SemaphoreType.DMA((-(-slots // (2 * GROUP)),)),
        ],
        compiler_params=pltpu.CompilerParams(vmem_limit_bytes=20 << 20),
        name="near_terms",
    )(place, outer, own, partner, fine_list, mid_list, in_hbm(ops))


TALL = 24
UNROLL = 8
FIRST = (3, 2, 2)


def far_kernel(
    place, listed_ref, table, uph, upl, fine_term, mid_term, dnh_hbm, dnl_hbm, ops_hbm, out,
    ops, dnh, dnl, tiles, rows, upper, chosen, top_col, upper_col, listed, sems, down_sems, list_sem,
):
    slots, n = ops.shape[0], ops.shape[1]
    list_load = pltpu.make_async_copy(listed_ref, listed, list_sem)
    list_load.start()
    loads = []
    for k, at in enumerate(range(0, n, TALL)):
        where = (slice(None), pl.ds(at, min(TALL, n - at)))
        loads.append(pltpu.make_async_copy(ops_hbm.at[where], ops.at[where], sems.at[k]))
    down_loads = [
        pltpu.make_async_copy(source, target, down_sems.at[k])
        for k, (source, target) in enumerate(((dnh_hbm, dnh), (dnl_hbm, dnl)))
    ]
    queue = loads + down_loads

    def begin(count):
        for _ in range(count):
            queue.pop(0).start()

    begin(FIRST[0])
    parents = PITCH - 8
    rows[pl.ds(parents, 8), :] = jnp.zeros((8, n), F32)
    upper[...] = jnp.zeros_like(upper)
    for i, line in enumerate(ORDER_0):
        at = LINE_ROWS * i
        tiles[0, pl.ds(24 * line, 24), :] = table[pl.ds(at, 24), :]
        tiles[2, pl.ds(24 * line, 24), :] = table[pl.ds(at + 24, 24), :]
        front, back = table[pl.ds(at + 48, 8), :], table[pl.ds(at + 56, 8), :]
        moved = (front, pltpu.roll(front, 128 - TAIL, 1), pltpu.roll(front, 128 - 2 * TAIL, 1))
        moved += (back, pltpu.roll(back, 128 - TAIL, 1), pltpu.roll(back, 128 - 2 * TAIL, 1))
        for g in range(3):
            tiles[1, pl.ds(24 * line + 8 * g, 8), :] = moved[2 * g]
            tiles[3, pl.ds(24 * line + 8 * g, 8), :] = moved[2 * g + 1]
    for q in range(4):
        for i in range(2):
            body, tail = [tiles[2 * i + k, pl.ds(q, parents, stride=4), :] for k in range(2)]
            at = pl.ds((2 * q + i) * PITCH, parents)
            rows[at, pl.ds(0, 128)] = body
            rows[at, pl.ds(128, n - 128)] = tail[:, : n - 128]
    begin(FIRST[1])
    total = None
    for o in range(8):
        both = jnp.concatenate(split(rows[pl.ds(o * PITCH, parents), :]), axis=0)
        term = mm_nt(both, uph[o])
        term = term[:parents] + term[parents:] + mm_nt(both[:parents], upl[o])
        total = term if total is None else total + term
    upper[pl.ds(0, parents), :] = total
    begin(FIRST[2])
    list_load.wait()

    def choose(j):
        for t in range(2):
            chosen[3 * j + t] = jnp.broadcast_to(rows[pl.ds(listed[t, j], 1), :], (8, n))
        chosen[3 * j + 2] = jnp.broadcast_to(upper[pl.ds(listed[2, j], 1), :], (8, n))

    def some(i, carry):
        for k in range(UNROLL):
            choose(i * UNROLL + k)
        return carry

    lax.fori_loop(0, slots // UNROLL, some, 0)
    for j in range(slots // UNROLL * UNROLL, slots):
        choose(j)
    begin(len(queue))

    def block(start, size):
        edges = [(at, min(8, size - at)) for at in range(0, size, 8)]
        sums = [[jnp.zeros((height, n), F32)] * 3 for _, height in edges]
        for j in range(slots):
            factors = [chosen[3 * j + t] for t in range(3)]
            for part, (at, height) in zip(sums, edges, strict=True):
                piece = ops[j, pl.ds(start + at, height), :]
                for t in range(3):
                    part[t] = part[t] + piece * factors[t][:height]
        for part, (at, height) in zip(sums, edges, strict=True):
            s0, s1, s2 = [jnp.sum(s, axis=1, keepdims=True) for s in part]
            lane = lax.broadcasted_iota(I32, (height, 128), 1)
            where = pl.ds(start + at, height)
            top_col[where, :] = jnp.where(lane == 0, s0, jnp.where(lane == 1, s1, 0.0))
            upper_col[where, :] = jnp.where(lane < 2, s2, 0.0)

    def step(i, carry):
        at = pl.multiple_of(i * TALL, TALL)
        where = (slice(None), pl.ds(at, TALL))
        pltpu.make_async_copy(ops_hbm.at[where], ops.at[where], sems.at[i]).wait()
        block(at, TALL)
        return carry

    lax.fori_loop(0, n // TALL, step, 0)
    if n % TALL:
        loads[-1].wait()
        block(n // TALL * TALL, n % TALL)
    for load in down_loads:
        load.wait()
    both = jnp.concatenate(split(upper_col[...]), axis=1)
    octant = lax.rem(place[0] * 2, 8)
    lane = lax.broadcasted_iota(I32, (n, 128), 1)
    from_upper = [halves(mm(dnh[octant + i], both) + mm(dnl[octant + i], both)) for i in range(2)]
    local_top = top_col[...] + jnp.where(lane == 0, from_upper[0], jnp.where(lane == 1, from_upper[1], 0.0))
    local_mid = lowered(local_top, dnh, dnl) + mid_term[...]
    local_mid = jnp.where(lane < 16, local_mid, 0.0)
    local_fine = lowered(local_mid, dnh, dnl) + fine_term[...]
    for i in range(out.shape[0]):
        out[i] = local_fine


def far_terms(place, listed, table, uph, upl, dnh, dnl, fine_term, mid_term, ops, copies):
    slots, n = ops.shape[0], ops.shape[1]
    parents = table.shape[0] // LINE_ROWS * 6
    vm, sm = pl.BlockSpec(memory_space=VMEM), pl.BlockSpec(memory_space=pltpu.SMEM)
    return pl.pallas_call(
        far_kernel,
        out_shape=VMEM((copies, n, 128), F32),
        in_specs=[sm] + [vm] * 6 + [pl.BlockSpec(memory_space=pltpu.HBM)] * 3,
        out_specs=vm,
        scratch_shapes=[
            pltpu.VMEM((slots, n, n), F32),
            pltpu.VMEM((8, n, n), BF16),
            pltpu.VMEM((8, n, n), BF16),
            pltpu.VMEM((4, 4 * parents, 128), F32),
            pltpu.VMEM((8 * PITCH, n), F32),
            pltpu.VMEM((parents + 8, n), F32),
            pltpu.VMEM((3 * slots, 8, n), F32),
            pltpu.VMEM((n, 128), F32),
            pltpu.VMEM((n, 128), F32),
            pltpu.SMEM(listed.shape, I32),
            pltpu.SemaphoreType.DMA((-(-n // TALL),)),
            pltpu.SemaphoreType.DMA((2,)),
            pltpu.SemaphoreType.DMA,
        ],
        compiler_params=pltpu.CompilerParams(vmem_limit_bytes=20 << 20),
        name="far_terms",
    )(
        place, listed, table, uph, upl, fine_term, mid_term,
        in_hbm(dnh), in_hbm(dnl), in_hbm(ops),
    )


def exponents():
    entries = []
    for degree in range(ORDER + 1):
        for along_x in range(degree, -1, -1):
            for along_y in range(degree - along_x, -1, -1):
                entries.append((along_x, along_y, degree - along_x - along_y))
    return entries


def monomial_kernel(powers, coords, high_ref, low_ref):
    value = None
    for axis in range(3):
        e = powers[:, pl.ds(axis, 1)]
        base = coords[pl.ds(axis, 1), :]
        for bit in range(4):
            factor = jnp.where((e >> bit) & 1 == 1, base, 1.0)
            value = factor if value is None else value * factor
            base = base * base
    high_ref[...], low_ref[...] = split(value)


def monomials(coords):
    table = jnp.asarray(exponents(), I32)
    n, particles = table.shape[0], coords.shape[1]
    width = 512
    return pl.pallas_call(
        monomial_kernel,
        grid=(particles // width,),
        out_shape=(pltpu.HBM((n, particles), BF16),) * 2,
        in_specs=[pl.BlockSpec((n, 3), lambda i: (0, 0)), pl.BlockSpec((3, width), lambda i: (0, i))],
        out_specs=(pl.BlockSpec((n, width), lambda i: (0, i)),) * 2,
        compiler_params=pltpu.CompilerParams(vmem_limit_bytes=4 << 20),
        name="monomials",
    )(table, coords)


def potential_kernel(place, parts, leaves, high_ref, low_ref, fine_ref, out):
    fine = parts[0] + parts[1] + parts[2] + parts[3]
    fine_ref[...] = fine
    fh, fl = split(jnp.transpose(fine))
    width = 512
    cell = lax.broadcasted_iota(I32, (128, width), 0) + place[0] * 128
    for k in range(out.shape[1] // width):
        at = pl.ds(k * width, width)
        mh, ml = high_ref[:, at], low_ref[:, at]
        values = mm(fh, mh) + mm(fl, mh) + mm(fh, ml)
        out[:, at] = jnp.sum(jnp.where(cell == leaves[:, at], values, 0.0), axis=0, keepdims=True)


def potentials(place, parts, leaves, high, low):
    n = parts.shape[1]
    particles = leaves.shape[1]
    vm = pl.BlockSpec(memory_space=VMEM)
    return pl.pallas_call(
        potential_kernel,
        out_shape=(jax.ShapeDtypeStruct((n, 128), F32), jax.ShapeDtypeStruct((1, particles), F32)),
        in_specs=[pl.BlockSpec(memory_space=pltpu.SMEM)] + [vm] * 4,
        out_specs=(vm,) * 2,
        compiler_params=pltpu.CompilerParams(vmem_limit_bytes=4 << 20),
        name="potentials",
    )(place, parts, leaves, high, low)


DOM = ("dom_0", "dom_1")
DOM_SUB = ("dom_0", "dom_1", "sub")


def exchanged(copies, axis, order=None):
    groups = None if order is None else [order]
    return lax.all_to_all(copies, axis, split_axis=0, concat_axis=0, tiled=True, axis_index_groups=groups)


def shards(
    fine_partial,
    upward_ops,
    interaction_ops,
    downward_ops,
    fine_list,
    mid_list,
    top_list,
    upper_list,
    positions,
    leaf_cell,
):
    subs, slabs = lax.axis_size("sub"), lax.axis_size(DOM)
    domain = lax.axis_index(DOM).astype(I32)
    place = domain.reshape(1)
    lists = (place, jnp.transpose(top_list), upper_list, fine_list, jnp.transpose(mid_list))
    uph, upl, listed, fine_list, mid_list = split_ops(upward_ops, lists=lists)
    dnh, dnl = split_ops(downward_ops, pltpu.HBM)
    parts = exchanged(part_copies(jnp.transpose(fine_partial, (1, 0, 2)), subs), "sub")
    own, tops = own_moments(parts, uph, upl, lax.axis_size(DOM[1]))
    line = exchanged(tops, DOM[1], ORDER_1)
    outer = lax.ppermute(own, DOM, [(i, i + 2 * (i % 2) - 1) for i in range(1, slabs - 1)])
    partner = lax.ppermute(own, DOM, [(i, i ^ 1) for i in range(slabs)])
    table = exchanged(line_copies(line, lax.axis_size(DOM[0])), DOM[0], ORDER_0)
    table = table.reshape(-1, table.shape[2])
    fine_term, mid_term = near_terms(place, outer, own, partner, fine_list, mid_list, interaction_ops)
    partial = far_terms(
        place, listed, table, uph, upl, dnh, dnl, fine_term, mid_term, interaction_ops, subs
    )
    high, low = monomials(positions)
    parts = exchanged(partial, "sub")
    local_fine, potential = potentials(place, parts, leaf_cell.reshape(1, -1), high, low)
    return local_fine, potential.reshape(-1)


def solution(mesh):
    torus = Mesh(
        mesh.devices.reshape(8, 24, mesh.shape["sub"]), ("dom_0", "dom_1", "sub")
    )
    return jax.shard_map(
        shards,
        mesh=torus,
        in_specs=(
            P("sub", None, DOM),
            P(),
            P("sub", None, None),
            P(),
            P("sub", DOM),
            P("sub", DOM),
            P("sub", DOM),
            P("sub", None),
            P(None, DOM_SUB),
            P(DOM_SUB),
        ),
        out_specs=(P(None, DOM), P(DOM_SUB)),
        check_vma=False,
    )
```

```python
import jax
import jax.numpy as jnp
from jax import lax
from jax.experimental import pallas as pl
from jax.experimental.pallas import tpu as pltpu
from jax.sharding import Mesh
from jax.sharding import PartitionSpec as P


ORDER = 8
F32, BF16, I32 = jnp.float32, jnp.bfloat16, jnp.int32
VMEM = pltpu.VMEM
ORDER_0 = [6, 7, 5, 4, 3, 2, 1, 0]
ORDER_1 = list(range(23, -1, -1))


def split(value):
    high = value.astype(BF16)
    return high, (value - high.astype(F32)).astype(BF16)


def in_hbm(value):
    return pltpu.with_memory_space_constraint(value, pltpu.HBM)


def halves(pair):
    return pair[:, :128] + pair[:, 128:]


def mm(a, b):
    return jnp.dot(a, b, preferred_element_type=F32)


def mm_nt(a, b):
    return lax.dot_general(a, b, (((1,), (1,)), ((), ())), preferred_element_type=F32)


def gathered(high, low, chosen):
    return jnp.concatenate([mm(high, chosen).astype(BF16), mm(low, chosen).astype(BF16)], axis=1)


def ones_where(shape, test):
    rows = lax.broadcasted_iota(I32, shape, 0)
    lanes = lax.broadcasted_iota(I32, shape, 1)
    return test(rows, lanes).astype(F32).astype(BF16)


def octant_sum(high, low, pair):
    lane = lax.broadcasted_iota(I32, (1, 256), 1) % 8
    total = None
    for o in range(8):
        term = mm(high[o], pair) + mm(low[o], pair)
        total = jnp.where(lane == o, term, 0.0 if total is None else total)
    return halves(total)


def raised(moments, uph, upl):
    summed = octant_sum(uph, upl, jnp.concatenate(split(moments), axis=1))
    parent = ones_where((128, 128), lambda r, c: r // 8 == c)
    high, low = split(summed)
    return mm(high, parent) + mm(low, parent)


def lowered(expansion, dnh, dnl):
    child = ones_where((128, 128), lambda r, c: c // 8 == r)
    return octant_sum(dnh, dnl, gathered(*split(expansion), child))


PITCH = 56


def prepare_kernel(
    place, part_hbm, up_hbm, top_hbm, upper_hbm, fine_hbm, mid_hbm, copies, high, low, listed, fine_out, mid_out,
    part, ups, top, upper, sems, store_sems, up_sems,
):
    pairs = [(part_hbm, part), (top_hbm, top), (upper_hbm, upper), (fine_hbm, fine_out), (mid_hbm, mid_out)]
    loads = [pltpu.make_async_copy(source, target, sems.at[k]) for k, (source, target) in enumerate(pairs)]
    up_loads = [pltpu.make_async_copy(up_hbm.at[:, o, :], ups.at[o], up_sems.at[o]) for o in range(8)]
    for load in loads + up_loads:
        load.start()
    loads[0].wait()
    stores = [pltpu.make_async_copy(part, copies.at[i], store_sems.at[i]) for i in range(copies.shape[0])]
    for store in stores:
        store.start()
    for load in loads[1:]:
        load.wait()
    cells = top[...]
    listed[pl.ds(0, 2), :] = jnp.where(cells >= 0, (cells & 7) * PITCH + (cells >> 3), PITCH - 8)
    cells = upper[...]
    cells = jnp.where(cells >= 0, cells, PITCH - 8).astype(F32).astype(BF16)
    here = ones_where((8, cells.shape[1]), lambda r, c: c == place[0] // 4)
    listed[pl.ds(2, 1), :] = mm_nt(here, cells)[:1].astype(I32)
    for o in range(8):
        up_loads[o].wait()
        high[o], low[o] = split(ups[o])
    for store in stores:
        store.wait()


def prepare(place, part, up, top_list, upper_list, fine_list, mid_list, copies):
    n = part.shape[0]
    vm, hbm = pl.BlockSpec(memory_space=VMEM), pl.BlockSpec(memory_space=pltpu.HBM)
    given = (part, jnp.transpose(up, (1, 0, 2)), top_list, upper_list, fine_list, mid_list)
    return pl.pallas_call(
        prepare_kernel,
        out_shape=(
            pltpu.HBM((copies, *part.shape), F32),
            VMEM((8, n, n), BF16),
            VMEM((8, n, n), BF16),
            VMEM((3, top_list.shape[1]), I32),
            VMEM(fine_list.shape, I32),
            VMEM(mid_list.shape, I32),
        ),
        in_specs=[pl.BlockSpec(memory_space=pltpu.SMEM)] + [hbm] * 6,
        out_specs=(hbm,) + (vm,) * 5,
        scratch_shapes=[
            pltpu.VMEM(part.shape, F32),
            pltpu.VMEM((8, n, n), F32),
            pltpu.VMEM(top_list.shape, I32),
            pltpu.VMEM(upper_list.shape, I32),
            pltpu.SemaphoreType.DMA((5,)),
            pltpu.SemaphoreType.DMA((copies,)),
            pltpu.SemaphoreType.DMA((8,)),
        ],
        compiler_params=pltpu.CompilerParams(vmem_limit_bytes=8 << 20),
        name="prepare",
    )(place, *(in_hbm(x) for x in given))


def split_kernel(ops_hbm, high, low, parts, sems):
    copies = [pltpu.make_async_copy(ops_hbm.at[:, o, :], parts.at[o], sems.at[o]) for o in range(8)]
    for copy in copies:
        copy.start()
    for o in range(8):
        copies[o].wait()
        high[o], low[o] = split(parts[o])


def split_down(ops):
    n = ops.shape[1]
    return pl.pallas_call(
        split_kernel,
        out_shape=(pltpu.HBM((8, n, n), BF16),) * 2,
        in_specs=[pl.BlockSpec(memory_space=pltpu.HBM)],
        out_specs=(pl.BlockSpec(memory_space=VMEM),) * 2,
        scratch_shapes=[pltpu.VMEM((8, n, n), F32), pltpu.SemaphoreType.DMA((8,))],
        compiler_params=pltpu.CompilerParams(vmem_limit_bytes=8 << 20),
        name="split_down",
    )(in_hbm(jnp.transpose(ops, (1, 0, 2))))


MID_AT = 168
SHIFT = 64
TAIL = 37
LINE_ROWS = 64


def packed(first, second):
    n = first.shape[1]
    blank = jnp.zeros((1, SHIFT - (n - 128)), F32)
    rests = jnp.concatenate([first[:, 128:], blank, second[:, 128:], blank], axis=1)
    return jnp.concatenate([first[:, :128], rests, second[:, :128]], axis=1)


def own_kernel(parts, uph, upl, own_ref, top_ref):
    n = parts.shape[1]
    fine = (parts[0] + parts[1] + parts[2] + parts[3])[:, 0, :]
    own_ref[pl.ds(0, n), :] = fine
    mid = raised(fine, uph, upl)
    rows = jnp.transpose(mid)[:16]
    own_ref[pl.ds(MID_AT, 16), :] = rows[:, :128]
    own_ref[pl.ds(MID_AT + 16, 16), pl.ds(0, n - 128)] = rows[:, 128:]
    rows = jnp.transpose(raised(mid, uph, upl))
    row = packed(rows[:1], rows[1:2])
    for i in range(top_ref.shape[0]):
        top_ref[i] = row


def own_moments(parts, uph, upl, copies):
    return pl.pallas_call(
        own_kernel,
        out_shape=(VMEM((MID_AT + 32, 128), F32), VMEM((copies, 1, 384), F32)),
        in_specs=[pl.BlockSpec(memory_space=VMEM)] * 3,
        out_specs=(pl.BlockSpec(memory_space=VMEM),) * 2,
        compiler_params=pltpu.CompilerParams(vmem_limit_bytes=4 << 20),
        name="own_moments",
    )(parts, uph, upl)


def line_kernel(line, out):
    rows = jnp.concatenate([line[ORDER_1.index(i)] for i in range(line.shape[0])], axis=0)
    first, second, third = [rows[8 * g : 8 * g + 8, 128:256] for g in range(3)]
    lane = lax.broadcasted_iota(I32, (8, 128), 1)

    def beside(one, two, three):
        return jnp.where(lane < TAIL, one, jnp.where(lane < 2 * TAIL, two, three))

    tails = (
        beside(first, pltpu.roll(first, 128 + TAIL - SHIFT, 1), pltpu.roll(second, 2 * TAIL, 1)),
        beside(pltpu.roll(second, SHIFT, 1), pltpu.roll(third, TAIL, 1), pltpu.roll(third, 2 * TAIL - SHIFT, 1)),
    )
    packed_rows = jnp.concatenate([rows[:, :128], rows[:, 256:], *tails], axis=0)
    for i in range(out.shape[0]):
        out[i] = packed_rows


def line_copies(line, copies):
    return pl.pallas_call(
        line_kernel,
        out_shape=jax.ShapeDtypeStruct((copies, LINE_ROWS, 128), F32),
        in_specs=[pl.BlockSpec(memory_space=VMEM)],
        out_specs=pl.BlockSpec(memory_space=VMEM),
        compiler_params=pltpu.CompilerParams(vmem_limit_bytes=2 << 20),
        name="line_copies",
    )(line)


GROUP = 4
TALL = 24


def near_kernel(place, outer, own, partner, fl, ml, ops_hbm, fine_out, mid_out, head, ops, full, rows, mids, mid_rows, xa, xb, acc_a, acc_b, sems):
    slots, n = ops.shape[0], ops.shape[1]
    groups = -(-slots // GROUP)
    size = [min(GROUP, slots - k * GROUP) for k in range(groups)]
    copies = []
    for k in range(0, groups, 2):
        at = pl.ds(k * GROUP, sum(size[k : k + 2]))
        copies.append(pltpu.make_async_copy(ops_hbm.at[at], ops.at[at], sems.at[k // 2]))
        copies[-1].start()
    rows[...] = jnp.zeros_like(rows)
    second = lax.rem(place[0], 2)
    for i, ref in ((2 * second, outer), (1, own), (2 - 2 * second, partner)):
        at = pl.ds(pl.multiple_of(16 * i, 16), 16)
        full[i] = ref[pl.ds(0, n), :]
        rows[at, pl.ds(0, 128)] = ref[pl.ds(MID_AT, 16), :]
        rows[at, pl.ds(128, n - 128)] = ref[pl.ds(MID_AT + 16, 16), pl.ds(0, n - 128)]
    mid = jnp.transpose(rows[...])[:n]
    mids[:, pl.ds(0, 128)], mids[:, pl.ds(128, 128)] = split(mid)
    anchor = place[0] * 128 - 128
    mid_anchor = place[0] * 16 - 16
    lane = lax.broadcasted_iota(I32, (1, 128), 1)
    part = (lane // 16) % 2 * 128
    listed = ml[...]
    listed = jnp.where(listed >= 0, listed - mid_anchor, -1).astype(F32).astype(BF16)
    spread = ones_where((16, 128), lambda r, c: c % 16 == r)
    mid_rows[...] = lax.dot_general(listed, spread, (((0,), (0,)), ((), ())), preferred_element_type=F32).astype(I32)
    acc_a[...] = jnp.zeros_like(acc_a)
    acc_b[...] = jnp.zeros_like(acc_b)

    def load(k, count, xs):
        row = jnp.full((1, 128), -1, I32)
        for jj in range(count):
            row = jnp.where(lane // 32 == jj, mid_rows[pl.ds(k * GROUP + jj, 1), :], row)
        row = jnp.where(row >= 0, row + part, -1)
        source = lax.broadcasted_iota(I32, (256, 128), 0)
        tile = mm(mids[...], (source == row).astype(F32).astype(BF16)).astype(BF16)
        for jj in range(count):
            xs[jj, :, pl.ds(128, 128)] = jnp.where(lane // 32 == jj, tile, jnp.zeros_like(tile))
            row = fl[pl.ds(k * GROUP + jj, 1), :]
            row = jnp.where(row >= 0, row - anchor, 512)
            index = jnp.broadcast_to(row & 127, (n, 128))
            got = jnp.zeros((n, 128), F32)
            for i in range(3):
                moved = jnp.take_along_axis(full[i], index, axis=1, mode="promise_in_bounds")
                got = jnp.where(row >> 7 == i, moved, got)
            xs[jj, :, pl.ds(0, 128)], xs[jj, :, pl.ds(256, 128)] = split(got)

    def use(k, count, xs):
        a = b = None
        for jj in range(count):
            oh, ol = split(ops[k * GROUP + jj])
            x = xs[jj]
            ta = mm(oh, x[:, :256]) + mm(ol, x[:, :256])
            tb = mm(oh, x[:, 256:])
            a = ta if a is None else a + ta
            b = tb if b is None else b + tb
        acc_a[...] += a
        acc_b[...] += b

    load(0, GROUP, xa)

    def ready(i):
        at = pl.ds(0, 2 * GROUP)
        if isinstance(i, int):
            copies[i].wait()
        else:
            pltpu.make_async_copy(ops_hbm.at[at], ops.at[at], sems.at[i]).wait()

    def step(i, carry):
        ready(i)
        load(2 * i + 1, GROUP, xb)
        use(2 * i, GROUP, xa)
        load(2 * i + 2, GROUP, xa)
        use(2 * i + 1, GROUP, xb)
        return carry

    steady = groups // 2 - 1
    lax.fori_loop(0, steady, step, 0)
    bufs = (xa, xb)
    for k in range(2 * steady, groups):
        if k % 2 == 0:
            ready(k // 2)
        if k + 1 < groups:
            load(k + 1, size[k + 1], bufs[(k + 1) % 2])
        use(k, size[k], bufs[k % 2])
    head[...] = ops[:, pl.ds(0, TALL), :]
    fine_out[...] = acc_a[:, pl.ds(0, 128)] + acc_b[...]
    folded = acc_a[:, pl.ds(128, 128)]
    for shift in (64, 32, 16):
        folded = folded + pltpu.roll(folded, shift, 1)
    mid_out[...] = folded


def near_terms(place, outer, own, partner, fine_list, mid_list, ops):
    slots, n = ops.shape[0], ops.shape[1]
    vm = pl.BlockSpec(memory_space=VMEM)
    return pl.pallas_call(
        near_kernel,
        out_shape=(VMEM((n, 128), F32),) * 2 + (VMEM((slots, TALL, n), F32),),
        in_specs=[pl.BlockSpec(memory_space=pltpu.SMEM)] + [vm] * 5 + [pl.BlockSpec(memory_space=pltpu.HBM)],
        out_specs=(vm,) * 3,
        scratch_shapes=[
            pltpu.VMEM((slots, n, n), F32),
            pltpu.VMEM((3, n, 128), F32),
            pltpu.VMEM((128, 256), F32),
            pltpu.VMEM((n, 256), BF16),
            pltpu.VMEM((slots, 128), I32),
            pltpu.VMEM((GROUP, n, 384), BF16),
            pltpu.VMEM((GROUP, n, 384), BF16),
            pltpu.VMEM((n, 256), F32),
            pltpu.VMEM((n, 128), F32),
            pltpu.SemaphoreType.DMA((-(-slots // (2 * GROUP)),)),
        ],
        compiler_params=pltpu.CompilerParams(vmem_limit_bytes=20 << 20),
        name="near_terms",
    )(place, outer, own, partner, fine_list, mid_list, in_hbm(ops))


UNROLL = 8
FIRST = (3, 2, 2)


def far_kernel(
    place, listed_ref, table, uph, upl, fine_term, mid_term, head, dnh_hbm, dnl_hbm, ops_hbm, out,
    ops, dnh, dnl, tiles, rows, upper, chosen, top_col, upper_col, listed, sems, down_sems, list_sem,
):
    slots, n = ops.shape[0], ops.shape[1]
    list_load = pltpu.make_async_copy(listed_ref, listed, list_sem)
    list_load.start()
    loads = []
    for k, at in enumerate(range(TALL, n, TALL)):
        where = (slice(None), pl.ds(at, min(TALL, n - at)))
        loads.append(pltpu.make_async_copy(ops_hbm.at[where], ops.at[where], sems.at[k]))
    down_loads = [
        pltpu.make_async_copy(source, target, down_sems.at[k])
        for k, (source, target) in enumerate(((dnh_hbm, dnh), (dnl_hbm, dnl)))
    ]
    queue = loads + down_loads

    def begin(count):
        for _ in range(count):
            queue.pop(0).start()

    begin(FIRST[0])
    parents = PITCH - 8
    rows[pl.ds(parents, 8), :] = jnp.zeros((8, n), F32)
    upper[...] = jnp.zeros_like(upper)
    for i, line in enumerate(ORDER_0):
        at = LINE_ROWS * i
        tiles[0, pl.ds(24 * line, 24), :] = table[pl.ds(at, 24), :]
        tiles[2, pl.ds(24 * line, 24), :] = table[pl.ds(at + 24, 24), :]
        front, back = table[pl.ds(at + 48, 8), :], table[pl.ds(at + 56, 8), :]
        moved = (front, pltpu.roll(front, 128 - TAIL, 1), pltpu.roll(front, 128 - 2 * TAIL, 1))
        moved += (back, pltpu.roll(back, 128 - TAIL, 1), pltpu.roll(back, 128 - 2 * TAIL, 1))
        for g in range(3):
            tiles[1, pl.ds(24 * line + 8 * g, 8), :] = moved[2 * g]
            tiles[3, pl.ds(24 * line + 8 * g, 8), :] = moved[2 * g + 1]
    for q in range(4):
        for i in range(2):
            body, tail = [tiles[2 * i + k, pl.ds(q, parents, stride=4), :] for k in range(2)]
            at = pl.ds((2 * q + i) * PITCH, parents)
            rows[at, pl.ds(0, 128)] = body
            rows[at, pl.ds(128, n - 128)] = tail[:, : n - 128]
    begin(FIRST[1])
    total = None
    for o in range(8):
        both = jnp.concatenate(split(rows[pl.ds(o * PITCH, parents), :]), axis=0)
        term = mm_nt(both, uph[o])
        term = term[:parents] + term[parents:] + mm_nt(both[:parents], upl[o])
        total = term if total is None else total + term
    upper[pl.ds(0, parents), :] = total
    begin(FIRST[2])
    list_load.wait()

    def choose(j):
        for t in range(2):
            chosen[3 * j + t] = jnp.broadcast_to(rows[pl.ds(listed[t, j], 1), :], (8, n))
        chosen[3 * j + 2] = jnp.broadcast_to(upper[pl.ds(listed[2, j], 1), :], (8, n))

    def some(i, carry):
        for k in range(UNROLL):
            choose(i * UNROLL + k)
        return carry

    lax.fori_loop(0, slots // UNROLL, some, 0)
    for j in range(slots // UNROLL * UNROLL, slots):
        choose(j)
    begin(len(queue))

    def block(start, size, source=ops):
        edges = [(at, min(8, size - at)) for at in range(0, size, 8)]
        sums = [[jnp.zeros((height, n), F32)] * 3 for _, height in edges]
        for j in range(slots):
            factors = [chosen[3 * j + t] for t in range(3)]
            for part, (at, height) in zip(sums, edges, strict=True):
                piece = source[j, pl.ds(start + at, height), :]
                for t in range(3):
                    part[t] = part[t] + piece * factors[t][:height]
        for part, (at, height) in zip(sums, edges, strict=True):
            s0, s1, s2 = [jnp.sum(s, axis=1, keepdims=True) for s in part]
            lane = lax.broadcasted_iota(I32, (height, 128), 1)
            where = pl.ds(start + at, height)
            top_col[where, :] = jnp.where(lane == 0, s0, jnp.where(lane == 1, s1, 0.0))
            upper_col[where, :] = jnp.where(lane < 2, s2, 0.0)

    def step(i, carry):
        at = pl.multiple_of(i * TALL, TALL)
        where = (slice(None), pl.ds(at, TALL))
        pltpu.make_async_copy(ops_hbm.at[where], ops.at[where], sems.at[i - 1]).wait()
        block(at, TALL)
        return carry

    block(0, TALL, head)
    lax.fori_loop(1, n // TALL, step, 0)
    if n % TALL:
        loads[-1].wait()
        block(n // TALL * TALL, n % TALL)
    for load in down_loads:
        load.wait()
    both = jnp.concatenate(split(upper_col[...]), axis=1)
    octant = lax.rem(place[0] * 2, 8)
    lane = lax.broadcasted_iota(I32, (n, 128), 1)
    from_upper = [halves(mm(dnh[octant + i], both) + mm(dnl[octant + i], both)) for i in range(2)]
    local_top = top_col[...] + jnp.where(lane == 0, from_upper[0], jnp.where(lane == 1, from_upper[1], 0.0))
    local_mid = lowered(local_top, dnh, dnl) + mid_term[...]
    local_mid = jnp.where(lane < 16, local_mid, 0.0)
    local_fine = lowered(local_mid, dnh, dnl) + fine_term[...]
    for i in range(out.shape[0]):
        out[i] = local_fine


def far_terms(place, listed, table, uph, upl, dnh, dnl, fine_term, mid_term, head, ops, copies):
    slots, n = ops.shape[0], ops.shape[1]
    parents = table.shape[0] // LINE_ROWS * 6
    vm, sm = pl.BlockSpec(memory_space=VMEM), pl.BlockSpec(memory_space=pltpu.SMEM)
    return pl.pallas_call(
        far_kernel,
        out_shape=VMEM((copies, n, 128), F32),
        in_specs=[sm] + [vm] * 7 + [pl.BlockSpec(memory_space=pltpu.HBM)] * 3,
        out_specs=vm,
        scratch_shapes=[
            pltpu.VMEM((slots, n, n), F32),
            pltpu.VMEM((8, n, n), BF16),
            pltpu.VMEM((8, n, n), BF16),
            pltpu.VMEM((4, 4 * parents, 128), F32),
            pltpu.VMEM((8 * PITCH, n), F32),
            pltpu.VMEM((parents + 8, n), F32),
            pltpu.VMEM((3 * slots, 8, n), F32),
            pltpu.VMEM((n, 128), F32),
            pltpu.VMEM((n, 128), F32),
            pltpu.SMEM(listed.shape, I32),
            pltpu.SemaphoreType.DMA((-(-n // TALL),)),
            pltpu.SemaphoreType.DMA((2,)),
            pltpu.SemaphoreType.DMA,
        ],
        compiler_params=pltpu.CompilerParams(vmem_limit_bytes=20 << 20),
        name="far_terms",
    )(
        place, listed, table, uph, upl, fine_term, mid_term, head,
        in_hbm(dnh), in_hbm(dnl), in_hbm(ops),
    )


def exponents():
    entries = []
    for degree in range(ORDER + 1):
        for along_x in range(degree, -1, -1):
            for along_y in range(degree - along_x, -1, -1):
                entries.append((along_x, along_y, degree - along_x - along_y))
    return entries


def monomial_kernel(powers, coords, high_ref, low_ref):
    value = None
    for axis in range(3):
        e = powers[:, pl.ds(axis, 1)]
        base = coords[pl.ds(axis, 1), :]
        for bit in range(4):
            factor = jnp.where((e >> bit) & 1 == 1, base, 1.0)
            value = factor if value is None else value * factor
            base = base * base
    high_ref[...], low_ref[...] = split(value)


def monomials(coords):
    table = jnp.asarray(exponents(), I32)
    n, particles = table.shape[0], coords.shape[1]
    width = 1024
    return pl.pallas_call(
        monomial_kernel,
        grid=(particles // width,),
        out_shape=(pltpu.HBM((n, particles), BF16),) * 2,
        in_specs=[pl.BlockSpec((n, 3), lambda i: (0, 0)), pl.BlockSpec((3, width), lambda i: (0, i))],
        out_specs=(pl.BlockSpec((n, width), lambda i: (0, i)),) * 2,
        compiler_params=pltpu.CompilerParams(vmem_limit_bytes=8 << 20),
        name="monomials",
    )(table, coords)


def potential_kernel(place, parts, leaves, high_ref, low_ref, fine_ref, out):
    fine = parts[0] + parts[1] + parts[2] + parts[3]
    fine_ref[...] = fine
    fh, fl = split(jnp.transpose(fine))
    width = 512
    cell = lax.broadcasted_iota(I32, (128, width), 0) + place[0] * 128
    for k in range(out.shape[1] // width):
        at = pl.ds(k * width, width)
        mh, ml = high_ref[:, at], low_ref[:, at]
        values = mm(fh, mh) + mm(fl, mh) + mm(fh, ml)
        out[:, at] = jnp.sum(jnp.where(cell == leaves[:, at], values, 0.0), axis=0, keepdims=True)


def potentials(place, parts, leaves, high, low):
    n = parts.shape[1]
    particles = leaves.shape[1]
    vm = pl.BlockSpec(memory_space=VMEM)
    return pl.pallas_call(
        potential_kernel,
        out_shape=(jax.ShapeDtypeStruct((n, 128), F32), jax.ShapeDtypeStruct((1, particles), F32)),
        in_specs=[pl.BlockSpec(memory_space=pltpu.SMEM)] + [vm] * 4,
        out_specs=(vm,) * 2,
        compiler_params=pltpu.CompilerParams(vmem_limit_bytes=4 << 20),
        name="potentials",
    )(place, parts, leaves, high, low)


DOM = ("dom_0", "dom_1")
DOM_SUB = ("dom_0", "dom_1", "sub")


def exchanged(copies, axis, order=None):
    groups = None if order is None else [order]
    return lax.all_to_all(copies, axis, split_axis=0, concat_axis=0, tiled=True, axis_index_groups=groups)


def shards(
    fine_partial,
    upward_ops,
    interaction_ops,
    downward_ops,
    fine_list,
    mid_list,
    top_list,
    upper_list,
    positions,
    leaf_cell,
):
    subs, slabs = lax.axis_size("sub"), lax.axis_size(DOM)
    domain = lax.axis_index(DOM).astype(I32)
    place = domain.reshape(1)
    copies, uph, upl, listed, fine_list, mid_list = prepare(
        place,
        jnp.transpose(fine_partial, (1, 0, 2)),
        upward_ops,
        jnp.transpose(top_list),
        upper_list,
        fine_list,
        jnp.transpose(mid_list),
        subs,
    )
    parts = exchanged(copies, "sub")
    own, tops = own_moments(parts, uph, upl, lax.axis_size(DOM[1]))
    line = exchanged(tops, DOM[1], ORDER_1)
    outer = lax.ppermute(own, DOM, [(i, i + 2 * (i % 2) - 1) for i in range(1, slabs - 1)])
    partner = lax.ppermute(own, DOM, [(i, i ^ 1) for i in range(slabs)])
    table = exchanged(line_copies(line, lax.axis_size(DOM[0])), DOM[0], ORDER_0)
    table = table.reshape(-1, table.shape[2])
    dnh, dnl = split_down(downward_ops)
    fine_term, mid_term, head = near_terms(place, outer, own, partner, fine_list, mid_list, interaction_ops)
    partial = far_terms(
        place, listed, table, uph, upl, dnh, dnl, fine_term, mid_term, head, interaction_ops, subs
    )
    high, low = monomials(positions)
    parts = exchanged(partial, "sub")
    local_fine, potential = potentials(place, parts, leaf_cell.reshape(1, -1), high, low)
    return local_fine, potential.reshape(-1)


def solution(mesh):
    torus = Mesh(
        mesh.devices.reshape(8, 24, mesh.shape["sub"]), ("dom_0", "dom_1", "sub")
    )
    return jax.shard_map(
        shards,
        mesh=torus,
        in_specs=(
            P("sub", None, DOM),
            P(),
            P("sub", None, None),
            P(),
            P("sub", DOM),
            P("sub", DOM),
            P("sub", DOM),
            P("sub", None),
            P(None, DOM_SUB),
            P(DOM_SUB),
        ),
        out_specs=(P(None, DOM), P(DOM_SUB)),
        check_vma=False,
    )
```

```python
import jax
import jax.numpy as jnp
from jax import lax
from jax.experimental import pallas as pl
from jax.experimental.pallas import tpu as pltpu
from jax.sharding import Mesh
from jax.sharding import PartitionSpec as P


ORDER = 8
F32, BF16, I32 = jnp.float32, jnp.bfloat16, jnp.int32
VMEM = pltpu.VMEM
ORDER_0 = [6, 0, 1, 2, 3, 4, 5, 7]
ORDER_1 = list(range(23, -1, -1))


def split(value):
    high = value.astype(BF16)
    return high, (value - high.astype(F32)).astype(BF16)


def in_hbm(value):
    return pltpu.with_memory_space_constraint(value, pltpu.HBM)


def halves(pair):
    return pair[:, :128] + pair[:, 128:]


def mm(a, b):
    return jnp.dot(a, b, preferred_element_type=F32)


def mm_nt(a, b):
    return lax.dot_general(a, b, (((1,), (1,)), ((), ())), preferred_element_type=F32)


def gathered(high, low, chosen):
    return jnp.concatenate([mm(high, chosen).astype(BF16), mm(low, chosen).astype(BF16)], axis=1)


def ones_where(shape, test):
    rows = lax.broadcasted_iota(I32, shape, 0)
    lanes = lax.broadcasted_iota(I32, shape, 1)
    return test(rows, lanes).astype(F32).astype(BF16)


def octant_sum(high, low, pair):
    lane = lax.broadcasted_iota(I32, (1, 256), 1) % 8
    total = None
    for o in range(8):
        term = mm(high[o], pair) + mm(low[o], pair)
        total = jnp.where(lane == o, term, 0.0 if total is None else total)
    return halves(total)


def raised(moments, uph, upl):
    summed = octant_sum(uph, upl, jnp.concatenate(split(moments), axis=1))
    parent = ones_where((128, 128), lambda r, c: r // 8 == c)
    high, low = split(summed)
    return mm(high, parent) + mm(low, parent)


def lowered(expansion, dnh, dnl):
    child = ones_where((128, 128), lambda r, c: c // 8 == r)
    return octant_sum(dnh, dnl, gathered(*split(expansion), child))


PITCH = 56


def prepare_kernel(
    place, part_hbm, up_hbm, top_hbm, upper_hbm, fine_hbm, mid_hbm, copies, high, low, listed, fine_out, mid_out,
    part, ups, top, upper, sems, store_sems, up_sems,
):
    pairs = [(part_hbm, part), (top_hbm, top), (upper_hbm, upper), (fine_hbm, fine_out), (mid_hbm, mid_out)]
    loads = [pltpu.make_async_copy(source, target, sems.at[k]) for k, (source, target) in enumerate(pairs)]
    up_loads = [pltpu.make_async_copy(up_hbm.at[:, o, :], ups.at[o], up_sems.at[o]) for o in range(8)]
    for load in loads + up_loads:
        load.start()
    loads[0].wait()
    stores = [pltpu.make_async_copy(part, copies.at[i], store_sems.at[i]) for i in range(copies.shape[0])]
    for store in stores:
        store.start()
    for load in loads[1:]:
        load.wait()
    cells = top[...]
    listed[pl.ds(0, 2), :] = jnp.where(cells >= 0, (cells & 7) * PITCH + (cells >> 3), PITCH - 8)
    cells = upper[...]
    cells = jnp.where(cells >= 0, cells, PITCH - 8).astype(F32).astype(BF16)
    here = ones_where((8, cells.shape[1]), lambda r, c: c == place[0] // 4)
    listed[pl.ds(2, 1), :] = mm_nt(here, cells)[:1].astype(I32)
    for o in range(8):
        up_loads[o].wait()
        high[o], low[o] = split(ups[o])
    for store in stores:
        store.wait()


def prepare(place, part, up, top_list, upper_list, fine_list, mid_list, copies):
    n = part.shape[0]
    vm, hbm = pl.BlockSpec(memory_space=VMEM), pl.BlockSpec(memory_space=pltpu.HBM)
    given = (part, jnp.transpose(up, (1, 0, 2)), top_list, upper_list, fine_list, mid_list)
    return pl.pallas_call(
        prepare_kernel,
        out_shape=(
            pltpu.HBM((copies, *part.shape), F32),
            VMEM((8, n, n), BF16),
            VMEM((8, n, n), BF16),
            VMEM((3, top_list.shape[1]), I32),
            VMEM(fine_list.shape, I32),
            VMEM(mid_list.shape, I32),
        ),
        in_specs=[pl.BlockSpec(memory_space=pltpu.SMEM)] + [hbm] * 6,
        out_specs=(hbm,) + (vm,) * 5,
        scratch_shapes=[
            pltpu.VMEM(part.shape, F32),
            pltpu.VMEM((8, n, n), F32),
            pltpu.VMEM(top_list.shape, I32),
            pltpu.VMEM(upper_list.shape, I32),
            pltpu.SemaphoreType.DMA((5,)),
            pltpu.SemaphoreType.DMA((copies,)),
            pltpu.SemaphoreType.DMA((8,)),
        ],
        compiler_params=pltpu.CompilerParams(vmem_limit_bytes=8 << 20),
        name="prepare",
    )(place, *(in_hbm(x) for x in given))


def split_kernel(ops_hbm, high, low, parts, sems):
    copies = [pltpu.make_async_copy(ops_hbm.at[:, o, :], parts.at[o], sems.at[o]) for o in range(8)]
    for copy in copies:
        copy.start()
    for o in range(8):
        copies[o].wait()
        high[o], low[o] = split(parts[o])


def split_down(ops):
    n = ops.shape[1]
    return pl.pallas_call(
        split_kernel,
        out_shape=(pltpu.HBM((8, n, n), BF16),) * 2,
        in_specs=[pl.BlockSpec(memory_space=pltpu.HBM)],
        out_specs=(pl.BlockSpec(memory_space=VMEM),) * 2,
        scratch_shapes=[pltpu.VMEM((8, n, n), F32), pltpu.SemaphoreType.DMA((8,))],
        compiler_params=pltpu.CompilerParams(vmem_limit_bytes=8 << 20),
        name="split_down",
    )(in_hbm(jnp.transpose(ops, (1, 0, 2))))


MID_AT = 168
SHIFT = 64
TAIL = 37
LINE_ROWS = 64


def packed(first, second):
    n = first.shape[1]
    blank = jnp.zeros((1, SHIFT - (n - 128)), F32)
    rests = jnp.concatenate([first[:, 128:], blank, second[:, 128:], blank], axis=1)
    return jnp.concatenate([first[:, :128], rests, second[:, :128]], axis=1)


def own_kernel(parts, uph, upl, own_ref, top_ref):
    n = parts.shape[1]
    fine = (parts[0] + parts[1] + parts[2] + parts[3])[:, 0, :]
    own_ref[pl.ds(0, n), :] = fine
    mid = raised(fine, uph, upl)
    rows = jnp.transpose(mid)[:16]
    own_ref[pl.ds(MID_AT, 16), :] = rows[:, :128]
    own_ref[pl.ds(MID_AT + 16, 16), pl.ds(0, n - 128)] = rows[:, 128:]
    rows = jnp.transpose(raised(mid, uph, upl))
    row = packed(rows[:1], rows[1:2])
    for i in range(top_ref.shape[0]):
        top_ref[i] = row


def own_moments(parts, uph, upl, copies):
    return pl.pallas_call(
        own_kernel,
        out_shape=(VMEM((MID_AT + 32, 128), F32), VMEM((copies, 1, 384), F32)),
        in_specs=[pl.BlockSpec(memory_space=VMEM)] * 3,
        out_specs=(pl.BlockSpec(memory_space=VMEM),) * 2,
        compiler_params=pltpu.CompilerParams(vmem_limit_bytes=4 << 20),
        name="own_moments",
    )(parts, uph, upl)


def line_kernel(line, out):
    rows = jnp.concatenate([line[ORDER_1.index(i)] for i in range(line.shape[0])], axis=0)
    first, second, third = [rows[8 * g : 8 * g + 8, 128:256] for g in range(3)]
    lane = lax.broadcasted_iota(I32, (8, 128), 1)

    def beside(one, two, three):
        return jnp.where(lane < TAIL, one, jnp.where(lane < 2 * TAIL, two, three))

    tails = (
        beside(first, pltpu.roll(first, 128 + TAIL - SHIFT, 1), pltpu.roll(second, 2 * TAIL, 1)),
        beside(pltpu.roll(second, SHIFT, 1), pltpu.roll(third, TAIL, 1), pltpu.roll(third, 2 * TAIL - SHIFT, 1)),
    )
    packed_rows = jnp.concatenate([rows[:, :128], rows[:, 256:], *tails], axis=0)
    for i in range(out.shape[0]):
        out[i] = packed_rows


def line_copies(line, copies):
    return pl.pallas_call(
        line_kernel,
        out_shape=jax.ShapeDtypeStruct((copies, LINE_ROWS, 128), F32),
        in_specs=[pl.BlockSpec(memory_space=VMEM)],
        out_specs=pl.BlockSpec(memory_space=VMEM),
        compiler_params=pltpu.CompilerParams(vmem_limit_bytes=2 << 20),
        name="line_copies",
    )(line)


GROUP = 4
TALL = 24


def near_kernel(place, outer, own, partner, fl, ml, ops_hbm, fine_out, mid_out, tails, ops, full, rows, mids, mid_rows, xa, xb, acc_a, acc_b, sems):
    slots, n = ops.shape[0], ops.shape[1]
    groups = -(-slots // GROUP)
    size = [min(GROUP, slots - k * GROUP) for k in range(groups)]
    copies = []
    for k in range(0, groups, 2):
        at = pl.ds(k * GROUP, sum(size[k : k + 2]))
        copies.append(pltpu.make_async_copy(ops_hbm.at[at], ops.at[at], sems.at[k // 2]))
        copies[-1].start()
    rows[...] = jnp.zeros_like(rows)
    second = lax.rem(place[0], 2)
    for i, ref in ((2 * second, outer), (1, own), (2 - 2 * second, partner)):
        at = pl.ds(pl.multiple_of(16 * i, 16), 16)
        full[i] = ref[pl.ds(0, n), :]
        rows[at, pl.ds(0, 128)] = ref[pl.ds(MID_AT, 16), :]
        rows[at, pl.ds(128, n - 128)] = ref[pl.ds(MID_AT + 16, 16), pl.ds(0, n - 128)]
    mid = jnp.transpose(rows[...])[:n]
    mids[:, pl.ds(0, 128)], mids[:, pl.ds(128, 128)] = split(mid)
    anchor = place[0] * 128 - 128
    mid_anchor = place[0] * 16 - 16
    lane = lax.broadcasted_iota(I32, (1, 128), 1)
    part = (lane // 16) % 2 * 128
    listed = ml[...]
    listed = jnp.where(listed >= 0, listed - mid_anchor, -1).astype(F32).astype(BF16)
    spread = ones_where((16, 128), lambda r, c: c % 16 == r)
    mid_rows[...] = lax.dot_general(listed, spread, (((0,), (0,)), ((), ())), preferred_element_type=F32).astype(I32)
    acc_a[...] = jnp.zeros_like(acc_a)
    acc_b[...] = jnp.zeros_like(acc_b)

    def load(k, count, xs):
        row = jnp.full((1, 128), -1, I32)
        for jj in range(count):
            row = jnp.where(lane // 32 == jj, mid_rows[pl.ds(k * GROUP + jj, 1), :], row)
        row = jnp.where(row >= 0, row + part, -1)
        source = lax.broadcasted_iota(I32, (256, 128), 0)
        tile = mm(mids[...], (source == row).astype(F32).astype(BF16)).astype(BF16)
        for jj in range(count):
            xs[jj, :, pl.ds(128, 128)] = jnp.where(lane // 32 == jj, tile, jnp.zeros_like(tile))
            row = fl[pl.ds(k * GROUP + jj, 1), :]
            row = jnp.where(row >= 0, row - anchor, 512)
            index = jnp.broadcast_to(row & 127, (n, 128))
            got = jnp.zeros((n, 128), F32)
            for i in range(3):
                moved = jnp.take_along_axis(full[i], index, axis=1, mode="promise_in_bounds")
                got = jnp.where(row >> 7 == i, moved, got)
            xs[jj, :, pl.ds(0, 128)], xs[jj, :, pl.ds(256, 128)] = split(got)

    def use(k, count, xs):
        a = b = None
        for jj in range(count):
            oh, ol = split(ops[k * GROUP + jj])
            x = xs[jj]
            ta = mm(oh, x[:, :256]) + mm(ol, x[:, :256])
            tb = mm(oh, x[:, 256:])
            a = ta if a is None else a + ta
            b = tb if b is None else b + tb
        acc_a[...] += a
        acc_b[...] += b

    load(0, GROUP, xa)

    def ready(i):
        at = pl.ds(0, 2 * GROUP)
        if isinstance(i, int):
            copies[i].wait()
        else:
            pltpu.make_async_copy(ops_hbm.at[at], ops.at[at], sems.at[i]).wait()

    def step(i, carry):
        ready(i)
        load(2 * i + 1, GROUP, xb)
        use(2 * i, GROUP, xa)
        load(2 * i + 2, GROUP, xa)
        use(2 * i + 1, GROUP, xb)
        return carry

    steady = groups // 2 - 1
    lax.fori_loop(0, steady, step, 0)
    bufs = (xa, xb)
    for k in range(2 * steady, groups):
        if k % 2 == 0:
            ready(k // 2)
        if k + 1 < groups:
            load(k + 1, size[k + 1], bufs[(k + 1) % 2])
        use(k, size[k], bufs[k % 2])
    for k in range(tails.shape[0]):
        parts = [ops[j, :, pl.ds(128, TAIL)] for j in range(3 * k, min(3 * k + 3, slots))]
        parts.append(jnp.zeros((n, 128 - TAIL * len(parts)), F32))
        tails[k] = jnp.concatenate(parts, axis=1)
    fine_out[...] = acc_a[:, pl.ds(0, 128)] + acc_b[...]
    folded = acc_a[:, pl.ds(128, 128)]
    for shift in (64, 32, 16):
        folded = folded + pltpu.roll(folded, shift, 1)
    mid_out[...] = folded


def near_terms(place, outer, own, partner, fine_list, mid_list, ops):
    slots, n = ops.shape[0], ops.shape[1]
    vm = pl.BlockSpec(memory_space=VMEM)
    return pl.pallas_call(
        near_kernel,
        out_shape=(VMEM((n, 128), F32),) * 2 + (VMEM((-(-slots // 3), n, 128), F32),),
        in_specs=[pl.BlockSpec(memory_space=pltpu.SMEM)] + [vm] * 5 + [pl.BlockSpec(memory_space=pltpu.HBM)],
        out_specs=(vm,) * 3,
        scratch_shapes=[
            pltpu.VMEM((slots, n, n), F32),
            pltpu.VMEM((3, n, 128), F32),
            pltpu.VMEM((128, 256), F32),
            pltpu.VMEM((n, 256), BF16),
            pltpu.VMEM((slots, 128), I32),
            pltpu.VMEM((GROUP, n, 384), BF16),
            pltpu.VMEM((GROUP, n, 384), BF16),
            pltpu.VMEM((n, 256), F32),
            pltpu.VMEM((n, 128), F32),
            pltpu.SemaphoreType.DMA((-(-slots // (2 * GROUP)),)),
        ],
        compiler_params=pltpu.CompilerParams(vmem_limit_bytes=20 << 20),
        name="near_terms",
    )(place, outer, own, partner, fine_list, mid_list, in_hbm(ops))


UNROLL = 1
FIRST = (3, 2, 2)


def far_kernel(
    place, listed_ref, table, uph, upl, fine_term, mid_term, tails, dnh_hbm, dnl_hbm, ops_hbm, out,
    ops, dnh, dnl, tiles, rows, upper, tail_rows, chosen, chosen_tails, top_col, upper_col, listed, sems, down_sems, list_sem,
):
    slots, n = ops.shape[0], ops.shape[1]
    triples = tails.shape[0]
    list_load = pltpu.make_async_copy(listed_ref, listed, list_sem)
    list_load.start()
    loads = []
    for k, at in enumerate(range(0, n, TALL)):
        where = (slice(None), pl.ds(at, min(TALL, n - at)), pl.ds(0, 128))
        loads.append(pltpu.make_async_copy(ops_hbm.at[where], ops.at[where[:2]], sems.at[k]))
    down_loads = [
        pltpu.make_async_copy(source, target, down_sems.at[k])
        for k, (source, target) in enumerate(((dnh_hbm, dnh), (dnl_hbm, dnl)))
    ]
    queue = loads + down_loads

    def begin(count):
        for _ in range(count):
            queue.pop(0).start()

    begin(FIRST[0])
    parents = PITCH - 8
    rows[pl.ds(parents, 8), :] = jnp.zeros((8, n), F32)
    upper[...] = jnp.zeros_like(upper)
    for i, line in enumerate(ORDER_0):
        at = LINE_ROWS * i
        tiles[0, pl.ds(24 * line, 24), :] = table[pl.ds(at, 24), :]
        tiles[2, pl.ds(24 * line, 24), :] = table[pl.ds(at + 24, 24), :]
        front, back = table[pl.ds(at + 48, 8), :], table[pl.ds(at + 56, 8), :]
        moved = (front, pltpu.roll(front, 128 - TAIL, 1), pltpu.roll(front, 128 - 2 * TAIL, 1))
        moved += (back, pltpu.roll(back, 128 - TAIL, 1), pltpu.roll(back, 128 - 2 * TAIL, 1))
        for g in range(3):
            tiles[1, pl.ds(24 * line + 8 * g, 8), :] = moved[2 * g]
            tiles[3, pl.ds(24 * line + 8 * g, 8), :] = moved[2 * g + 1]
    for q in range(4):
        for i in range(2):
            body, tail = [tiles[2 * i + k, pl.ds(q, parents, stride=4), :] for k in range(2)]
            at = pl.ds((2 * q + i) * PITCH, parents)
            rows[at, pl.ds(0, 128)] = body
            rows[at, pl.ds(128, n - 128)] = tail[:, : n - 128]
    begin(FIRST[1])
    total = None
    for o in range(8):
        both = jnp.concatenate(split(rows[pl.ds(o * PITCH, parents), :]), axis=0)
        term = mm_nt(both, uph[o])
        term = term[:parents] + term[parents:] + mm_nt(both[:parents], upl[o])
        total = term if total is None else total + term
    upper[pl.ds(0, parents), :] = total
    begin(FIRST[2])
    list_load.wait()
    lane = lax.broadcasted_iota(I32, (1, 128), 1)
    for source, at in ((rows, 0), (upper, rows.shape[0])):
        size = source.shape[0]
        rest = jnp.concatenate([source[:, pl.ds(128, TAIL)], jnp.zeros((size, 128 - TAIL), F32)], axis=1)
        for i in range(3):
            tail_rows[i, pl.ds(at, size), :] = pltpu.roll(rest, TAIL * i, 1) if i else rest

    def choose(k, count):
        for t in range(3):
            source, shift = (rows, 0) if t < 2 else (upper, rows.shape[0])
            tail = None
            for i in range(count):
                index = listed[t, 3 * k + i]
                chosen[9 * k + 3 * i + t] = jnp.broadcast_to(source[pl.ds(index, 1), :][:, :128], (8, 128))
                part = tail_rows[i, pl.ds(index + shift, 1), :]
                tail = part if tail is None else tail + part
            chosen_tails[3 * k + t] = jnp.broadcast_to(tail, (8, 128))

    def some(i, carry):
        for k in range(UNROLL):
            choose(i * UNROLL + k, 3)
        return carry

    lax.fori_loop(0, slots // 3 // UNROLL, some, 0)
    for k in range(slots // 3 // UNROLL * UNROLL, triples):
        choose(k, min(3, slots - 3 * k))
    begin(len(queue))

    def block(start, size):
        edges = [(at, min(8, size - at)) for at in range(0, size, 8)]
        sums = [[jnp.zeros((height, 128), F32)] * 3 for _, height in edges]

        def add(pieces, factors):
            for part, piece, (_, height) in zip(sums, pieces, edges, strict=True):
                for t in range(3):
                    part[t] = part[t] + piece * factors[t][:height]

        for j in range(slots):
            add([ops[j, pl.ds(start + at, height), :] for at, height in edges], [chosen[3 * j + t] for t in range(3)])
        for k in range(triples):
            add(
                [tails[k, pl.ds(start + at, height), :] for at, height in edges],
                [chosen_tails[3 * k + t] for t in range(3)],
            )
        for part, (at, height) in zip(sums, edges, strict=True):
            s0, s1, s2 = [jnp.sum(s, axis=1, keepdims=True) for s in part]
            lane = lax.broadcasted_iota(I32, (height, 128), 1)
            where = pl.ds(start + at, height)
            top_col[where, :] = jnp.where(lane == 0, s0, jnp.where(lane == 1, s1, 0.0))
            upper_col[where, :] = jnp.where(lane < 2, s2, 0.0)

    def step(i, carry):
        at = pl.multiple_of(i * TALL, TALL)
        where = (slice(None), pl.ds(at, TALL), pl.ds(0, 128))
        pltpu.make_async_copy(ops_hbm.at[where], ops.at[where[:2]], sems.at[i]).wait()
        block(at, TALL)
        return carry

    lax.fori_loop(0, n // TALL, step, 0)
    if n % TALL:
        loads[-1].wait()
        block(n // TALL * TALL, n % TALL)
    for load in down_loads:
        load.wait()
    both = jnp.concatenate(split(upper_col[...]), axis=1)
    octant = lax.rem(place[0] * 2, 8)
    lane = lax.broadcasted_iota(I32, (n, 128), 1)
    from_upper = [halves(mm(dnh[octant + i], both) + mm(dnl[octant + i], both)) for i in range(2)]
    local_top = top_col[...] + jnp.where(lane == 0, from_upper[0], jnp.where(lane == 1, from_upper[1], 0.0))
    local_mid = lowered(local_top, dnh, dnl) + mid_term[...]
    local_mid = jnp.where(lane < 16, local_mid, 0.0)
    local_fine = lowered(local_mid, dnh, dnl) + fine_term[...]
    for i in range(out.shape[0]):
        out[i] = local_fine


def far_terms(place, listed, table, uph, upl, dnh, dnl, fine_term, mid_term, tails, ops, copies):
    slots, n = ops.shape[0], ops.shape[1]
    parents = table.shape[0] // LINE_ROWS * 6
    vm, sm = pl.BlockSpec(memory_space=VMEM), pl.BlockSpec(memory_space=pltpu.SMEM)
    return pl.pallas_call(
        far_kernel,
        out_shape=VMEM((copies, n, 128), F32),
        in_specs=[sm] + [vm] * 7 + [pl.BlockSpec(memory_space=pltpu.HBM)] * 3,
        out_specs=vm,
        scratch_shapes=[
            pltpu.VMEM((slots, n, 128), F32),
            pltpu.VMEM((8, n, n), BF16),
            pltpu.VMEM((8, n, n), BF16),
            pltpu.VMEM((4, 4 * parents, 128), F32),
            pltpu.VMEM((8 * PITCH, n), F32),
            pltpu.VMEM((parents + 8, n), F32),
            pltpu.VMEM((3, 8 * PITCH + parents + 8, 128), F32),
            pltpu.VMEM((3 * slots, 8, 128), F32),
            pltpu.VMEM((slots + 3, 8, 128), F32),
            pltpu.VMEM((n, 128), F32),
            pltpu.VMEM((n, 128), F32),
            pltpu.SMEM(listed.shape, I32),
            pltpu.SemaphoreType.DMA((-(-n // TALL),)),
            pltpu.SemaphoreType.DMA((2,)),
            pltpu.SemaphoreType.DMA,
        ],
        compiler_params=pltpu.CompilerParams(vmem_limit_bytes=20 << 20),
        name="far_terms",
    )(
        place, listed, table, uph, upl, fine_term, mid_term, tails,
        in_hbm(dnh), in_hbm(dnl), in_hbm(ops),
    )


def exponents():
    entries = []
    for degree in range(ORDER + 1):
        for along_x in range(degree, -1, -1):
            for along_y in range(degree - along_x, -1, -1):
                entries.append((along_x, along_y, degree - along_x - along_y))
    return entries


def monomial_kernel(powers, coords, high_ref, low_ref):
    value = None
    for axis in range(3):
        e = powers[:, pl.ds(axis, 1)]
        base = coords[pl.ds(axis, 1), :]
        for bit in range(4):
            factor = jnp.where((e >> bit) & 1 == 1, base, 1.0)
            value = factor if value is None else value * factor
            base = base * base
    high_ref[...], low_ref[...] = split(value)


def monomials(coords):
    table = jnp.asarray(exponents(), I32)
    n, particles = table.shape[0], coords.shape[1]
    width = 1024
    return pl.pallas_call(
        monomial_kernel,
        grid=(particles // width,),
        out_shape=(pltpu.HBM((n, particles), BF16),) * 2,
        in_specs=[pl.BlockSpec((n, 3), lambda i: (0, 0)), pl.BlockSpec((3, width), lambda i: (0, i))],
        out_specs=(pl.BlockSpec((n, width), lambda i: (0, i)),) * 2,
        compiler_params=pltpu.CompilerParams(vmem_limit_bytes=8 << 20),
        name="monomials",
    )(table, coords)


def potential_kernel(place, parts, leaves, high_ref, low_ref, fine_ref, out):
    fine = parts[0] + parts[1] + parts[2] + parts[3]
    fine_ref[...] = fine
    fh, fl = split(jnp.transpose(fine))
    width = 512
    cell = lax.broadcasted_iota(I32, (128, width), 0) + place[0] * 128
    for k in range(out.shape[1] // width):
        at = pl.ds(k * width, width)
        mh, ml = high_ref[:, at], low_ref[:, at]
        values = mm(fh, mh) + mm(fl, mh) + mm(fh, ml)
        out[:, at] = jnp.sum(jnp.where(cell == leaves[:, at], values, 0.0), axis=0, keepdims=True)


def potentials(place, parts, leaves, high, low):
    n = parts.shape[1]
    particles = leaves.shape[1]
    vm = pl.BlockSpec(memory_space=VMEM)
    return pl.pallas_call(
        potential_kernel,
        out_shape=(jax.ShapeDtypeStruct((n, 128), F32), jax.ShapeDtypeStruct((1, particles), F32)),
        in_specs=[pl.BlockSpec(memory_space=pltpu.SMEM)] + [vm] * 4,
        out_specs=(vm,) * 2,
        compiler_params=pltpu.CompilerParams(vmem_limit_bytes=4 << 20),
        name="potentials",
    )(place, parts, leaves, high, low)


DOM = ("dom_0", "dom_1")
DOM_SUB = ("dom_0", "dom_1", "sub")


def exchanged(copies, axis, order=None):
    groups = None if order is None else [order]
    return lax.all_to_all(copies, axis, split_axis=0, concat_axis=0, tiled=True, axis_index_groups=groups)


def shards(
    fine_partial,
    upward_ops,
    interaction_ops,
    downward_ops,
    fine_list,
    mid_list,
    top_list,
    upper_list,
    positions,
    leaf_cell,
):
    subs, slabs = lax.axis_size("sub"), lax.axis_size(DOM)
    domain = lax.axis_index(DOM).astype(I32)
    place = domain.reshape(1)
    copies, uph, upl, listed, fine_list, mid_list = prepare(
        place,
        jnp.transpose(fine_partial, (1, 0, 2)),
        upward_ops,
        jnp.transpose(top_list),
        upper_list,
        fine_list,
        jnp.transpose(mid_list),
        subs,
    )
    parts = exchanged(copies, "sub")
    own, tops = own_moments(parts, uph, upl, lax.axis_size(DOM[1]))
    line = exchanged(tops, DOM[1], ORDER_1)
    outer = lax.ppermute(own, DOM, [(i, i + 2 * (i % 2) - 1) for i in range(1, slabs - 1)])
    partner = lax.ppermute(own, DOM, [(i, i ^ 1) for i in range(slabs)])
    table = exchanged(line_copies(line, lax.axis_size(DOM[0])), DOM[0], ORDER_0)
    table = table.reshape(-1, table.shape[2])
    dnh, dnl = split_down(downward_ops)
    fine_term, mid_term, head = near_terms(place, outer, own, partner, fine_list, mid_list, interaction_ops)
    partial = far_terms(
        place, listed, table, uph, upl, dnh, dnl, fine_term, mid_term, head, interaction_ops, subs
    )
    high, low = monomials(positions)
    parts = exchanged(partial, "sub")
    local_fine, potential = potentials(place, parts, leaf_cell.reshape(1, -1), high, low)
    return local_fine, potential.reshape(-1)


def solution(mesh):
    torus = Mesh(
        mesh.devices.reshape(8, 24, mesh.shape["sub"]), ("dom_0", "dom_1", "sub")
    )
    return jax.shard_map(
        shards,
        mesh=torus,
        in_specs=(
            P("sub", None, DOM),
            P(),
            P("sub", None, None),
            P(),
            P("sub", DOM),
            P("sub", DOM),
            P("sub", DOM),
            P("sub", None),
            P(None, DOM_SUB),
            P(DOM_SUB),
        ),
        out_specs=(P(None, DOM), P(DOM_SUB)),
        check_vma=False,
    )
```

```python
import jax
import jax.numpy as jnp
from jax import lax
from jax.experimental import pallas as pl
from jax.experimental.pallas import tpu as pltpu
from jax.sharding import Mesh
from jax.sharding import PartitionSpec as P


ORDER = 8
F32, BF16, I32 = jnp.float32, jnp.bfloat16, jnp.int32
VMEM = pltpu.VMEM
ORDER_0 = [6, 0, 1, 2, 3, 4, 5, 7]
ORDER_1 = list(range(23, -1, -1))


def split(value):
    high = value.astype(BF16)
    return high, (value - high.astype(F32)).astype(BF16)


def in_hbm(value):
    return pltpu.with_memory_space_constraint(value, pltpu.HBM)


def halves(pair):
    return pair[:, :128] + pair[:, 128:]


def mm(a, b):
    return jnp.dot(a, b, preferred_element_type=F32)


def mm_nt(a, b):
    return lax.dot_general(a, b, (((1,), (1,)), ((), ())), preferred_element_type=F32)


def gathered(high, low, chosen):
    return jnp.concatenate([mm(high, chosen).astype(BF16), mm(low, chosen).astype(BF16)], axis=1)


def ones_where(shape, test):
    rows = lax.broadcasted_iota(I32, shape, 0)
    lanes = lax.broadcasted_iota(I32, shape, 1)
    return test(rows, lanes).astype(F32).astype(BF16)


def octant_sum(high, low, pair):
    lane = lax.broadcasted_iota(I32, (1, 256), 1) % 8
    total = None
    for o in range(8):
        term = mm(high[o], pair) + mm(low[o], pair)
        total = jnp.where(lane == o, term, 0.0 if total is None else total)
    return halves(total)


def raised(moments, uph, upl):
    summed = octant_sum(uph, upl, jnp.concatenate(split(moments), axis=1))
    parent = ones_where((128, 128), lambda r, c: r // 8 == c)
    high, low = split(summed)
    return mm(high, parent) + mm(low, parent)


def lowered(expansion, dnh, dnl):
    child = ones_where((128, 128), lambda r, c: c // 8 == r)
    return octant_sum(dnh, dnl, gathered(*split(expansion), child))


PITCH = 56


def prepare_kernel(
    place, part_hbm, up_hbm, top_hbm, upper_hbm, fine_hbm, mid_hbm, copies, high, low, listed, fine_out, mid_out,
    part, ups, top, upper, sems, store_sems, up_sems,
):
    pairs = [(part_hbm, part), (top_hbm, top), (upper_hbm, upper), (fine_hbm, fine_out), (mid_hbm, mid_out)]
    loads = [pltpu.make_async_copy(source, target, sems.at[k]) for k, (source, target) in enumerate(pairs)]
    up_loads = [pltpu.make_async_copy(up_hbm.at[:, o, :], ups.at[o], up_sems.at[o]) for o in range(8)]
    for load in loads + up_loads:
        load.start()
    loads[0].wait()
    stores = [pltpu.make_async_copy(part, copies.at[i], store_sems.at[i]) for i in range(copies.shape[0])]
    for store in stores:
        store.start()
    for load in loads[1:]:
        load.wait()
    cells = top[...]
    listed[pl.ds(0, 2), :] = jnp.where(cells >= 0, (cells & 7) * PITCH + (cells >> 3), PITCH - 8)
    cells = upper[...]
    cells = jnp.where(cells >= 0, cells, PITCH - 8).astype(F32).astype(BF16)
    here = ones_where((8, cells.shape[1]), lambda r, c: c == place[0] // 4)
    listed[pl.ds(2, 1), :] = mm_nt(here, cells)[:1].astype(I32)
    for o in range(8):
        up_loads[o].wait()
        high[o], low[o] = split(ups[o])
    for store in stores:
        store.wait()


def prepare(place, part, up, top_list, upper_list, fine_list, mid_list, copies):
    n = part.shape[0]
    vm, hbm = pl.BlockSpec(memory_space=VMEM), pl.BlockSpec(memory_space=pltpu.HBM)
    given = (part, jnp.transpose(up, (1, 0, 2)), top_list, upper_list, fine_list, mid_list)
    return pl.pallas_call(
        prepare_kernel,
        out_shape=(
            pltpu.HBM((copies, *part.shape), F32),
            VMEM((8, n, n), BF16),
            VMEM((8, n, n), BF16),
            VMEM((3, top_list.shape[1]), I32),
            VMEM(fine_list.shape, I32),
            VMEM(mid_list.shape, I32),
        ),
        in_specs=[pl.BlockSpec(memory_space=pltpu.SMEM)] + [hbm] * 6,
        out_specs=(hbm,) + (vm,) * 5,
        scratch_shapes=[
            pltpu.VMEM(part.shape, F32),
            pltpu.VMEM((8, n, n), F32),
            pltpu.VMEM(top_list.shape, I32),
            pltpu.VMEM(upper_list.shape, I32),
            pltpu.SemaphoreType.DMA((5,)),
            pltpu.SemaphoreType.DMA((copies,)),
            pltpu.SemaphoreType.DMA((8,)),
        ],
        compiler_params=pltpu.CompilerParams(vmem_limit_bytes=8 << 20),
        name="prepare",
    )(place, *(in_hbm(x) for x in given))


def split_kernel(ops_hbm, high, low, parts, sems):
    copies = [pltpu.make_async_copy(ops_hbm.at[:, o, :], parts.at[o], sems.at[o]) for o in range(8)]
    for copy in copies:
        copy.start()
    for o in range(8):
        copies[o].wait()
        high[o], low[o] = split(parts[o])


def split_down(ops):
    n = ops.shape[1]
    return pl.pallas_call(
        split_kernel,
        out_shape=(pltpu.HBM((8, n, n), BF16),) * 2,
        in_specs=[pl.BlockSpec(memory_space=pltpu.HBM)],
        out_specs=(pl.BlockSpec(memory_space=VMEM),) * 2,
        scratch_shapes=[pltpu.VMEM((8, n, n), F32), pltpu.SemaphoreType.DMA((8,))],
        compiler_params=pltpu.CompilerParams(vmem_limit_bytes=8 << 20),
        name="split_down",
    )(in_hbm(jnp.transpose(ops, (1, 0, 2))))


MID_AT = 168
SHIFT = 64
TAIL = 37
LINE_ROWS = 64


def packed(first, second):
    n = first.shape[1]
    blank = jnp.zeros((1, SHIFT - (n - 128)), F32)
    rests = jnp.concatenate([first[:, 128:], blank, second[:, 128:], blank], axis=1)
    return jnp.concatenate([first[:, :128], rests, second[:, :128]], axis=1)


def own_kernel(parts, uph, upl, own_ref, top_ref):
    n = parts.shape[1]
    fine = (parts[0] + parts[1] + parts[2] + parts[3])[:, 0, :]
    own_ref[pl.ds(0, n), :] = fine
    mid = raised(fine, uph, upl)
    rows = jnp.transpose(mid)[:16]
    own_ref[pl.ds(MID_AT, 16), :] = rows[:, :128]
    own_ref[pl.ds(MID_AT + 16, 16), pl.ds(0, n - 128)] = rows[:, 128:]
    rows = jnp.transpose(octant_sum(uph, upl, jnp.concatenate(split(mid), axis=1)))
    row = packed(*(jnp.sum(rows[8 * i : 8 * i + 8], axis=0, keepdims=True) for i in range(2)))
    for i in range(top_ref.shape[0]):
        top_ref[i] = row


def own_moments(parts, uph, upl, copies):
    return pl.pallas_call(
        own_kernel,
        out_shape=(VMEM((MID_AT + 32, 128), F32), VMEM((copies, 1, 384), F32)),
        in_specs=[pl.BlockSpec(memory_space=VMEM)] * 3,
        out_specs=(pl.BlockSpec(memory_space=VMEM),) * 2,
        compiler_params=pltpu.CompilerParams(vmem_limit_bytes=4 << 20),
        name="own_moments",
    )(parts, uph, upl)


def line_kernel(line, out):
    rows = jnp.concatenate([line[ORDER_1.index(i)] for i in range(line.shape[0])], axis=0)
    first, second, third = [rows[8 * g : 8 * g + 8, 128:256] for g in range(3)]
    lane = lax.broadcasted_iota(I32, (8, 128), 1)

    def beside(one, two, three):
        return jnp.where(lane < TAIL, one, jnp.where(lane < 2 * TAIL, two, three))

    tails = (
        beside(first, pltpu.roll(first, 128 + TAIL - SHIFT, 1), pltpu.roll(second, 2 * TAIL, 1)),
        beside(pltpu.roll(second, SHIFT, 1), pltpu.roll(third, TAIL, 1), pltpu.roll(third, 2 * TAIL - SHIFT, 1)),
    )
    packed_rows = jnp.concatenate([rows[:, :128], rows[:, 256:], *tails], axis=0)
    for i in range(out.shape[0]):
        out[i] = packed_rows


def line_copies(line, copies):
    return pl.pallas_call(
        line_kernel,
        out_shape=jax.ShapeDtypeStruct((copies, LINE_ROWS, 128), F32),
        in_specs=[pl.BlockSpec(memory_space=VMEM)],
        out_specs=pl.BlockSpec(memory_space=VMEM),
        compiler_params=pltpu.CompilerParams(vmem_limit_bytes=2 << 20),
        name="line_copies",
    )(line)


GROUP = 4
TALL = 88


def near_kernel(place, outer, own, partner, fl, ml, ops_hbm, fine_out, mid_out, tails, ops, full, rows, mids, mid_rows, xa, xb, acc_a, acc_b, sems):
    slots, n = ops.shape[0], ops.shape[1]
    groups = -(-slots // GROUP)
    size = [min(GROUP, slots - k * GROUP) for k in range(groups)]
    copies = []
    for k in range(0, groups, 2):
        at = pl.ds(k * GROUP, sum(size[k : k + 2]))
        copies.append(pltpu.make_async_copy(ops_hbm.at[at], ops.at[at], sems.at[k // 2]))
        copies[-1].start()
    rows[...] = jnp.zeros_like(rows)
    second = lax.rem(place[0], 2)
    for i, ref in ((2 * second, outer), (1, own), (2 - 2 * second, partner)):
        at = pl.ds(pl.multiple_of(16 * i, 16), 16)
        full[i] = ref[pl.ds(0, n), :]
        rows[at, pl.ds(0, 128)] = ref[pl.ds(MID_AT, 16), :]
        rows[at, pl.ds(128, n - 128)] = ref[pl.ds(MID_AT + 16, 16), pl.ds(0, n - 128)]
    mid = jnp.transpose(rows[...])[:n]
    mids[:, pl.ds(0, 128)], mids[:, pl.ds(128, 128)] = split(mid)
    anchor = place[0] * 128 - 128
    mid_anchor = place[0] * 16 - 16
    lane = lax.broadcasted_iota(I32, (1, 128), 1)
    part = (lane // 16) % 2 * 128
    listed = ml[...]
    listed = jnp.where(listed >= 0, listed - mid_anchor, -1).astype(F32).astype(BF16)
    spread = ones_where((16, 128), lambda r, c: c % 16 == r)
    mid_rows[...] = lax.dot_general(listed, spread, (((0,), (0,)), ((), ())), preferred_element_type=F32).astype(I32)
    acc_a[...] = jnp.zeros_like(acc_a)
    acc_b[...] = jnp.zeros_like(acc_b)

    def load(k, count, xs):
        row = jnp.full((1, 128), -1, I32)
        for jj in range(count):
            row = jnp.where(lane // 32 == jj, mid_rows[pl.ds(k * GROUP + jj, 1), :], row)
        row = jnp.where(row >= 0, row + part, -1)
        source = lax.broadcasted_iota(I32, (256, 128), 0)
        tile = mm(mids[...], (source == row).astype(F32).astype(BF16)).astype(BF16)
        for jj in range(count):
            xs[jj, :, pl.ds(128, 128)] = jnp.where(lane // 32 == jj, tile, jnp.zeros_like(tile))
            row = fl[pl.ds(k * GROUP + jj, 1), :]
            row = jnp.where(row >= 0, row - anchor, 512)
            index = jnp.broadcast_to(row & 127, (n, 128))
            got = jnp.zeros((n, 128), F32)
            for i in range(3):
                moved = jnp.take_along_axis(full[i], index, axis=1, mode="promise_in_bounds")
                got = jnp.where(row >> 7 == i, moved, got)
            xs[jj, :, pl.ds(0, 128)], xs[jj, :, pl.ds(256, 128)] = split(got)

    def use(k, count, xs):
        a = b = None
        for jj in range(count):
            oh, ol = split(ops[k * GROUP + jj])
            x = xs[jj]
            ta = mm(oh, x[:, :256]) + mm(ol, x[:, :256])
            tb = mm(oh, x[:, 256:])
            a = ta if a is None else a + ta
            b = tb if b is None else b + tb
        acc_a[...] += a
        acc_b[...] += b

    load(0, GROUP, xa)

    def ready(i):
        at = pl.ds(0, 2 * GROUP)
        if isinstance(i, int):
            copies[i].wait()
        else:
            pltpu.make_async_copy(ops_hbm.at[at], ops.at[at], sems.at[i]).wait()

    def step(i, carry):
        ready(i)
        load(2 * i + 1, GROUP, xb)
        use(2 * i, GROUP, xa)
        load(2 * i + 2, GROUP, xa)
        use(2 * i + 1, GROUP, xb)
        return carry

    steady = groups // 2 - 1
    lax.fori_loop(0, steady, step, 0)
    bufs = (xa, xb)
    for k in range(2 * steady, groups):
        if k % 2 == 0:
            ready(k // 2)
        if k + 1 < groups:
            load(k + 1, size[k + 1], bufs[(k + 1) % 2])
        use(k, size[k], bufs[k % 2])
    for k in range(tails.shape[0]):
        parts = [ops[j, :, pl.ds(128, TAIL)] for j in range(3 * k, min(3 * k + 3, slots))]
        parts.append(jnp.zeros((n, 128 - TAIL * len(parts)), F32))
        tails[k] = jnp.concatenate(parts, axis=1)
    fine_out[...] = acc_a[:, pl.ds(0, 128)] + acc_b[...]
    folded = acc_a[:, pl.ds(128, 128)]
    for shift in (64, 32, 16):
        folded = folded + pltpu.roll(folded, shift, 1)
    mid_out[...] = folded


def near_terms(place, outer, own, partner, fine_list, mid_list, ops):
    slots, n = ops.shape[0], ops.shape[1]
    vm = pl.BlockSpec(memory_space=VMEM)
    return pl.pallas_call(
        near_kernel,
        out_shape=(VMEM((n, 128), F32),) * 2 + (VMEM((-(-slots // 3), n, 128), F32),),
        in_specs=[pl.BlockSpec(memory_space=pltpu.SMEM)] + [vm] * 5 + [pl.BlockSpec(memory_space=pltpu.HBM)],
        out_specs=(vm,) * 3,
        scratch_shapes=[
            pltpu.VMEM((slots, n, n), F32),
            pltpu.VMEM((3, n, 128), F32),
            pltpu.VMEM((128, 256), F32),
            pltpu.VMEM((n, 256), BF16),
            pltpu.VMEM((slots, 128), I32),
            pltpu.VMEM((GROUP, n, 384), BF16),
            pltpu.VMEM((GROUP, n, 384), BF16),
            pltpu.VMEM((n, 256), F32),
            pltpu.VMEM((n, 128), F32),
            pltpu.SemaphoreType.DMA((-(-slots // (2 * GROUP)),)),
        ],
        compiler_params=pltpu.CompilerParams(vmem_limit_bytes=20 << 20),
        name="near_terms",
    )(place, outer, own, partner, fine_list, mid_list, in_hbm(ops))


UNROLL = 1
FIRST = (4, 0, 0)


def far_kernel(
    place, listed_ref, table, uph, upl, fine_term, mid_term, tails, dnh_hbm, dnl_hbm, ops_hbm, out,
    ops, dnh, dnl, tiles, rows, upper, tail_rows, chosen, chosen_tails, top_col, upper_col, listed, sems, down_sems, list_sem,
):
    slots, n = ops.shape[0], ops.shape[1]
    triples = tails.shape[0]
    list_load = pltpu.make_async_copy(listed_ref, listed, list_sem)
    list_load.start()
    loads = []
    for k, at in enumerate(range(0, n, TALL)):
        where = (slice(None), pl.ds(at, min(TALL, n - at)), pl.ds(0, 128))
        loads.append(pltpu.make_async_copy(ops_hbm.at[where], ops.at[where[:2]], sems.at[k]))
    down_loads = [
        pltpu.make_async_copy(source, target, down_sems.at[k])
        for k, (source, target) in enumerate(((dnh_hbm, dnh), (dnl_hbm, dnl)))
    ]
    queue = loads + down_loads

    def begin(count):
        for _ in range(count):
            queue.pop(0).start()

    begin(FIRST[0])
    parents = PITCH - 8
    rows[pl.ds(parents, 8), :] = jnp.zeros((8, n), F32)
    upper[...] = jnp.zeros_like(upper)
    for i, line in enumerate(ORDER_0):
        at = LINE_ROWS * i
        tiles[0, pl.ds(24 * line, 24), :] = table[pl.ds(at, 24), :]
        tiles[2, pl.ds(24 * line, 24), :] = table[pl.ds(at + 24, 24), :]
        front, back = table[pl.ds(at + 48, 8), :], table[pl.ds(at + 56, 8), :]
        moved = (front, pltpu.roll(front, 128 - TAIL, 1), pltpu.roll(front, 128 - 2 * TAIL, 1))
        moved += (back, pltpu.roll(back, 128 - TAIL, 1), pltpu.roll(back, 128 - 2 * TAIL, 1))
        for g in range(3):
            tiles[1, pl.ds(24 * line + 8 * g, 8), :] = moved[2 * g]
            tiles[3, pl.ds(24 * line + 8 * g, 8), :] = moved[2 * g + 1]
    for q in range(4):
        for i in range(2):
            body, tail = [tiles[2 * i + k, pl.ds(q, parents, stride=4), :] for k in range(2)]
            at = pl.ds((2 * q + i) * PITCH, parents)
            rows[at, pl.ds(0, 128)] = body
            rows[at, pl.ds(128, n - 128)] = tail[:, : n - 128]
    begin(FIRST[1])
    total = None
    for o in range(8):
        both = jnp.concatenate(split(rows[pl.ds(o * PITCH, parents), :]), axis=0)
        term = mm_nt(both, uph[o])
        term = term[:parents] + term[parents:] + mm_nt(both[:parents], upl[o])
        total = term if total is None else total + term
    upper[pl.ds(0, parents), :] = total
    begin(FIRST[2])
    list_load.wait()
    lane = lax.broadcasted_iota(I32, (1, 128), 1)
    for source, at in ((rows, 0), (upper, rows.shape[0])):
        size = source.shape[0]
        rest = jnp.concatenate([source[:, pl.ds(128, TAIL)], jnp.zeros((size, 128 - TAIL), F32)], axis=1)
        for i in range(3):
            tail_rows[i, pl.ds(at, size), :] = pltpu.roll(rest, TAIL * i, 1) if i else rest

    def choose(k, count):
        for t in range(3):
            source, shift = (rows, 0) if t < 2 else (upper, rows.shape[0])
            tail = None
            for i in range(count):
                index = listed[t, 3 * k + i]
                chosen[9 * k + 3 * i + t] = jnp.broadcast_to(source[pl.ds(index, 1), :][:, :128], (8, 128))
                part = tail_rows[i, pl.ds(index + shift, 1), :]
                tail = part if tail is None else tail + part
            chosen_tails[3 * k + t] = jnp.broadcast_to(tail, (8, 128))

    def some(i, carry):
        for k in range(UNROLL):
            choose(i * UNROLL + k, 3)
        return carry

    lax.fori_loop(0, slots // 3 // UNROLL, some, 0)
    for k in range(slots // 3 // UNROLL * UNROLL, triples):
        choose(k, min(3, slots - 3 * k))
    begin(len(queue))

    def block(start, size):
        edges = [(at, min(8, size - at)) for at in range(0, size, 8)]
        sums = [[jnp.zeros((height, 128), F32)] * 3 for _, height in edges]

        def add(pieces, factors):
            for part, piece, (_, height) in zip(sums, pieces, edges, strict=True):
                for t in range(3):
                    part[t] = part[t] + piece * factors[t][:height]

        for j in range(slots):
            add([ops[j, pl.ds(start + at, height), :] for at, height in edges], [chosen[3 * j + t] for t in range(3)])
        for k in range(triples):
            add(
                [tails[k, pl.ds(start + at, height), :] for at, height in edges],
                [chosen_tails[3 * k + t] for t in range(3)],
            )
        for part, (at, height) in zip(sums, edges, strict=True):
            s0, s1, s2 = [jnp.sum(s, axis=1, keepdims=True) for s in part]
            lane = lax.broadcasted_iota(I32, (height, 128), 1)
            where = pl.ds(start + at, height)
            top_col[where, :] = jnp.where(lane == 0, s0, jnp.where(lane == 1, s1, 0.0))
            upper_col[where, :] = jnp.where(lane < 2, s2, 0.0)

    def step(i, carry):
        at = pl.multiple_of(i * TALL, TALL)
        where = (slice(None), pl.ds(at, TALL), pl.ds(0, 128))
        pltpu.make_async_copy(ops_hbm.at[where], ops.at[where[:2]], sems.at[i]).wait()
        block(at, TALL)
        return carry

    lax.fori_loop(0, n // TALL, step, 0)
    if n % TALL:
        loads[-1].wait()
        block(n // TALL * TALL, n % TALL)
    for load in down_loads:
        load.wait()
    both = jnp.concatenate(split(upper_col[...]), axis=1)
    octant = lax.rem(place[0] * 2, 8)
    lane = lax.broadcasted_iota(I32, (n, 128), 1)
    from_upper = [halves(mm(dnh[octant + i], both) + mm(dnl[octant + i], both)) for i in range(2)]
    local_top = top_col[...] + jnp.where(lane == 0, from_upper[0], jnp.where(lane == 1, from_upper[1], 0.0))
    local_mid = lowered(local_top, dnh, dnl) + mid_term[...]
    local_mid = jnp.where(lane < 16, local_mid, 0.0)
    local_fine = lowered(local_mid, dnh, dnl) + fine_term[...]
    for i in range(out.shape[0]):
        out[i] = local_fine


def far_terms(place, listed, table, uph, upl, dnh, dnl, fine_term, mid_term, tails, ops, copies):
    slots, n = ops.shape[0], ops.shape[1]
    parents = table.shape[0] // LINE_ROWS * 6
    vm, sm = pl.BlockSpec(memory_space=VMEM), pl.BlockSpec(memory_space=pltpu.SMEM)
    return pl.pallas_call(
        far_kernel,
        out_shape=VMEM((copies, n, 128), F32),
        in_specs=[sm] + [vm] * 7 + [pl.BlockSpec(memory_space=pltpu.HBM)] * 3,
        out_specs=vm,
        scratch_shapes=[
            pltpu.VMEM((slots, n, 128), F32),
            pltpu.VMEM((8, n, n), BF16),
            pltpu.VMEM((8, n, n), BF16),
            pltpu.VMEM((4, 4 * parents, 128), F32),
            pltpu.VMEM((8 * PITCH, n), F32),
            pltpu.VMEM((parents + 8, n), F32),
            pltpu.VMEM((3, 8 * PITCH + parents + 8, 128), F32),
            pltpu.VMEM((3 * slots, 8, 128), F32),
            pltpu.VMEM((slots + 3, 8, 128), F32),
            pltpu.VMEM((n, 128), F32),
            pltpu.VMEM((n, 128), F32),
            pltpu.SMEM(listed.shape, I32),
            pltpu.SemaphoreType.DMA((-(-n // TALL),)),
            pltpu.SemaphoreType.DMA((2,)),
            pltpu.SemaphoreType.DMA,
        ],
        compiler_params=pltpu.CompilerParams(vmem_limit_bytes=20 << 20),
        name="far_terms",
    )(
        place, listed, table, uph, upl, fine_term, mid_term, tails,
        in_hbm(dnh), in_hbm(dnl), in_hbm(ops),
    )


def exponents():
    entries = []
    for degree in range(ORDER + 1):
        for along_x in range(degree, -1, -1):
            for along_y in range(degree - along_x, -1, -1):
                entries.append((along_x, along_y, degree - along_x - along_y))
    return entries


def monomial_kernel(powers, coords, high_ref, low_ref):
    value = None
    for axis in range(3):
        e = powers[:, pl.ds(axis, 1)]
        base = coords[pl.ds(axis, 1), :]
        for bit in range(4):
            factor = jnp.where((e >> bit) & 1 == 1, base, 1.0)
            value = factor if value is None else value * factor
            base = base * base
    high_ref[...], low_ref[...] = split(value)


def monomials(coords):
    table = jnp.asarray(exponents(), I32)
    n, particles = table.shape[0], coords.shape[1]
    width = 1024
    return pl.pallas_call(
        monomial_kernel,
        grid=(particles // width,),
        out_shape=(pltpu.HBM((n, particles), BF16),) * 2,
        in_specs=[pl.BlockSpec((n, 3), lambda i: (0, 0)), pl.BlockSpec((3, width), lambda i: (0, i))],
        out_specs=(pl.BlockSpec((n, width), lambda i: (0, i)),) * 2,
        compiler_params=pltpu.CompilerParams(vmem_limit_bytes=8 << 20),
        name="monomials",
    )(table, coords)


def potential_kernel(place, parts, leaves, high_ref, low_ref, fine_ref, out):
    fine = parts[0] + parts[1] + parts[2] + parts[3]
    fine_ref[...] = fine
    fh, fl = split(jnp.transpose(fine))
    width = 512
    cell = lax.broadcasted_iota(I32, (128, width), 0) + place[0] * 128
    for k in range(out.shape[1] // width):
        at = pl.ds(k * width, width)
        mh, ml = high_ref[:, at], low_ref[:, at]
        values = mm(fh, mh) + mm(fl, mh) + mm(fh, ml)
        out[:, at] = jnp.sum(jnp.where(cell == leaves[:, at], values, 0.0), axis=0, keepdims=True)


def potentials(place, parts, leaves, high, low):
    n = parts.shape[1]
    particles = leaves.shape[1]
    vm = pl.BlockSpec(memory_space=VMEM)
    return pl.pallas_call(
        potential_kernel,
        out_shape=(jax.ShapeDtypeStruct((n, 128), F32), jax.ShapeDtypeStruct((1, particles), F32)),
        in_specs=[pl.BlockSpec(memory_space=pltpu.SMEM)] + [vm] * 4,
        out_specs=(vm,) * 2,
        compiler_params=pltpu.CompilerParams(vmem_limit_bytes=4 << 20),
        name="potentials",
    )(place, parts, leaves, high, low)


DOM = ("dom_0", "dom_1")
DOM_SUB = ("dom_0", "dom_1", "sub")


def exchanged(copies, axis, order=None):
    groups = None if order is None else [order]
    return lax.all_to_all(copies, axis, split_axis=0, concat_axis=0, tiled=True, axis_index_groups=groups)


def shards(
    fine_partial,
    upward_ops,
    interaction_ops,
    downward_ops,
    fine_list,
    mid_list,
    top_list,
    upper_list,
    positions,
    leaf_cell,
):
    subs, slabs = lax.axis_size("sub"), lax.axis_size(DOM)
    domain = lax.axis_index(DOM).astype(I32)
    place = domain.reshape(1)
    copies, uph, upl, listed, fine_list, mid_list = prepare(
        place,
        jnp.transpose(fine_partial, (1, 0, 2)),
        upward_ops,
        jnp.transpose(top_list),
        upper_list,
        fine_list,
        jnp.transpose(mid_list),
        subs,
    )
    parts = exchanged(copies, "sub")
    own, tops = own_moments(parts, uph, upl, lax.axis_size(DOM[1]))
    line = exchanged(tops, DOM[1], ORDER_1)
    outer = lax.ppermute(own, DOM, [(i, i + 2 * (i % 2) - 1) for i in range(1, slabs - 1)])
    partner = lax.ppermute(own, DOM, [(i, i ^ 1) for i in range(slabs)])
    table = exchanged(line_copies(line, lax.axis_size(DOM[0])), DOM[0], ORDER_0)
    table = table.reshape(-1, table.shape[2])
    dnh, dnl = split_down(downward_ops)
    fine_term, mid_term, head = near_terms(place, outer, own, partner, fine_list, mid_list, interaction_ops)
    partial = far_terms(
        place, listed, table, uph, upl, dnh, dnl, fine_term, mid_term, head, interaction_ops, subs
    )
    high, low = monomials(positions)
    parts = exchanged(partial, "sub")
    local_fine, potential = potentials(place, parts, leaf_cell.reshape(1, -1), high, low)
    return local_fine, potential.reshape(-1)


def solution(mesh):
    torus = Mesh(
        mesh.devices.reshape(8, 24, mesh.shape["sub"]), ("dom_0", "dom_1", "sub")
    )
    return jax.shard_map(
        shards,
        mesh=torus,
        in_specs=(
            P("sub", None, DOM),
            P(),
            P("sub", None, None),
            P(),
            P("sub", DOM),
            P("sub", DOM),
            P("sub", DOM),
            P("sub", None),
            P(None, DOM_SUB),
            P(DOM_SUB),
        ),
        out_specs=(P(None, DOM), P(DOM_SUB)),
        check_vma=False,
    )
```
